32 devices in a mesh: px: 4 (over x, core), py: 2 (over y), pz: 4 (over z).
Axes of the slice: x: 2, y: 2, z: 4, core: 2. Of those that a mesh axis runs over, the one named last changes fastest.
Arguments:
- control_values: float32 [28, 14, 28, 512], P('px', 'py', 'pz'), may hold values from -6 to 6
- metric_diag: float32 [3, 32, 512], P(None, 'px', ('py', 'pz')), may hold values from 0.5 to 2
- metric_off: float32 [3, 32, 512], P(None, 'px', ('py', 'pz')), may hold values from -0.2 to 0.2
- mass_weight: float32 [32, 512], P('px', ('py', 'pz')), may hold values from 0.5 to 2
- orient: int32 [4, 2, 4, 3], P('px', 'py', 'pz'), may hold values from 0 to 1
Outputs:
- stiffness_out: float32 [28, 14, 28, 512], P('px', 'py', 'pz')
- mass_out: float32 [28, 14, 28, 512], P('px', 'py', 'pz')
The draws below stay inside these ranges and needn't reach their ends.
All inputs are finite; a program needn't handle non-finite values.
Results may differ from the reference program's by a relative error of at most 0.0003.
Values sent between devices are 32-bit elements; how exact they have to be, the bound alone decides.
No kernel may reach another device: no remote copies, remote signals or barrier semaphores. Data moves between devices by JAX's collectives and lax.ppermute only.
A program may use at most 64 MiB of HBM per device.

```python
import math
import jax
import jax.numpy as jnp
import numpy as np
from jax import lax

ELEMS = 4
VECS = 512
CTRL = 7
QUAD = 8
N_PX = 4
N_PY = 2
N_PZ = 4


def touch_ends(drawn, own_key, smallest, top_value):
    shape = drawn.shape
    index_at = [jax.random.randint(jax.random.fold_in(own_key, axis), (), 0, shape[axis]) for axis in range(len(shape))]
    drawn = drawn.at[tuple(index_at)].set(smallest)
    longest = shape.index(max(shape))
    index_at[longest] = (index_at[longest] + 1) % shape[longest]
    return drawn.at[tuple(index_at)].set(top_value)


def levels(rng, dims, split, least, high):
    loudness = 1.0
    for axis_at, blocks in split:
        draws = jax.random.uniform(jax.random.fold_in(jax.random.fold_in(rng, 6), axis_at), (blocks,), jnp.float32, least / len(split), high / len(split))
        loudness = loudness * jnp.repeat(jnp.exp(draws), dims[axis_at] // blocks).reshape((-1,) + (1,) * (len(dims) - 1 - axis_at))
    return loudness


def bell_draw(stream_key, shape, deviation, most, split=(), held_as=jnp.bfloat16):
    result = deviation * jax.random.normal(stream_key, shape, jnp.float32)
    if split:
        result = result * levels(stream_key, shape, split, -0.22, 0.18)
    return jnp.clip(result, -most, most).astype(held_as)


def setup_inputs(seed: int = 0) -> dict:
    key_of = jax.random.split(jax.random.key(seed), 6)
    return {
        "control_values": bell_draw(key_of[0], (N_PX * CTRL, N_PY * CTRL, N_PZ * CTRL, VECS), 1.0, 6.0, ((0, 4), (1, 2), (2, 4)), jnp.float32),
        "metric_diag": jnp.clip(jnp.exp(math.log(2.0) - 1.3862944 * jax.random.uniform(key_of[1], (3, N_PX * QUAD, N_PY * N_PZ * QUAD * QUAD), jnp.float32) ** levels(key_of[1], (3, N_PX * QUAD, N_PY * N_PZ * QUAD * QUAD), ((1, 4), (2, 8)), -0.2, 0.2)), 0.5, 2.0),
        "metric_off": jnp.clip(jax.random.uniform(key_of[2], (3, N_PX * QUAD, N_PY * N_PZ * QUAD * QUAD), jnp.float32, -0.2, 0.2) * levels(key_of[2], (3, N_PX * QUAD, N_PY * N_PZ * QUAD * QUAD), ((1, 4), (2, 8)), -0.4, 0.0), -0.2, 0.2),
        "mass_weight": jnp.clip(jnp.exp(math.log(2.0) - 1.3862944 * jax.random.uniform(key_of[3], (N_PX * QUAD, N_PY * N_PZ * QUAD * QUAD), jnp.float32) ** levels(key_of[3], (N_PX * QUAD, N_PY * N_PZ * QUAD * QUAD), ((0, 4), (1, 8)), -0.2, 0.2)), 0.5, 2.0),
        "orient": touch_ends(jax.random.randint(key_of[4], (N_PX, N_PY, N_PZ, 3), 0, 2), jax.random.fold_in(key_of[4], 1), 0, 1).astype(jnp.int32),
    }


def spline_tables(elements):
    knot_row = np.concatenate([np.zeros(3), np.arange(elements + 1) * 1.0, np.full(3, float(elements))])
    offsets = np.array([0.5 - 0.5 / math.sqrt(3.0), 0.5 + 0.5 / math.sqrt(3.0)])
    points = (np.arange(elements)[:, None] + offsets[None, :]).reshape(-1)
    intervals = np.repeat(np.arange(elements), 2) + 3
    current = np.zeros((points.size, knot_row.size - 1))
    current[np.arange(points.size), intervals] = 1.0
    previous = current
    for degree in range(1, 4):
        columns = knot_row.size - 1 - degree
        updated = np.zeros((points.size, columns))
        for i in range(columns):
            lower_gap = knot_row[i + degree] - knot_row[i]
            upper_gap = knot_row[i + degree + 1] - knot_row[i + 1]
            if lower_gap > 0:
                updated[:, i] += (points - knot_row[i]) / lower_gap * current[:, i]
            if upper_gap > 0:
                updated[:, i] += (knot_row[i + degree + 1] - points) / upper_gap * current[:, i + 1]
        previous = current
        current = updated
    slopes = np.zeros(current.shape)
    for i in range(current.shape[1]):
        lower_gap = knot_row[i + 3] - knot_row[i]
        upper_gap = knot_row[i + 4] - knot_row[i + 1]
        if lower_gap > 0:
            slopes[:, i] += 3.0 / lower_gap * previous[:, i]
        if upper_gap > 0:
            slopes[:, i] -= 3.0 / upper_gap * previous[:, i + 1]
    return (current.astype(np.float32), slopes.astype(np.float32))

def contract(pattern, operand, table_part):
    return jnp.einsum(pattern, operand, table_part, precision=lax.Precision.HIGHEST)

def forward_parts(coeffs, values, slopes):
    along_b = contract('ijkv,ck->ijcv', coeffs, values)
    along_d = contract('ijkv,ck->ijcv', coeffs, slopes)
    plain = contract('ijcv,bj->ibcv', along_b, values)
    slope_y = contract('ijcv,bj->ibcv', along_b, slopes)
    slope_z = contract('ijcv,bj->ibcv', along_d, values)
    return (plain, slope_y, slope_z)

def stiffness_apply(parts, diag_terms, off_terms, values, slopes, block_rows):
    plain, slope_y, slope_z = parts
    quad_count = values.shape[0]
    back_x = jnp.zeros(plain.shape, jnp.float32)
    back_y = jnp.zeros(plain.shape, jnp.float32)
    back_z = jnp.zeros(plain.shape, jnp.float32)
    for first_row in range(0, quad_count, block_rows):
        last_row = first_row + block_rows
        slope_rows = slopes[first_row:last_row]
        value_rows = values[first_row:last_row]
        grad_x = contract('ibcv,ai->abcv', plain, slope_rows)
        grad_y = contract('ibcv,ai->abcv', slope_y, value_rows)
        grad_z = contract('ibcv,ai->abcv', slope_z, value_rows)
        diag_rows = diag_terms[:, first_row:last_row, :, :, None]
        off_rows = off_terms[:, first_row:last_row, :, :, None]
        flux_x = diag_rows[0] * grad_x + off_rows[0] * grad_y + off_rows[1] * grad_z
        flux_y = off_rows[0] * grad_x + diag_rows[1] * grad_y + off_rows[2] * grad_z
        flux_z = off_rows[1] * grad_x + off_rows[2] * grad_y + diag_rows[2] * grad_z
        back_x = back_x + contract('abcv,ai->ibcv', flux_x, slope_rows)
        back_y = back_y + contract('abcv,ai->ibcv', flux_y, value_rows)
        back_z = back_z + contract('abcv,ai->ibcv', flux_z, value_rows)
    middle_b = contract('ibcv,bj->ijcv', back_x, values) + contract('ibcv,bj->ijcv', back_y, slopes)
    middle_d = contract('ibcv,bj->ijcv', back_z, values)
    return contract('ijcv,ck->ijkv', middle_b, values) + contract('ijcv,ck->ijkv', middle_d, slopes)

def mass_apply(plain, weights, values, block_rows):
    quad_count = values.shape[0]
    back_mass = jnp.zeros(plain.shape, jnp.float32)
    for first_row in range(0, quad_count, block_rows):
        last_row = first_row + block_rows
        value_rows = values[first_row:last_row]
        point_values = contract('ibcv,ai->abcv', plain, value_rows)
        weighted = weights[first_row:last_row, :, :, None] * point_values
        back_mass = back_mass + contract('abcv,ai->ibcv', weighted, value_rows)
    middle = contract('ibcv,bj->ijcv', back_mass, values)
    return contract('ijcv,ck->ijkv', middle, values)

def flip_frame(grid_data, flip_flags, first_dim):
    for d in range(3):
        grid_data = jnp.where(flip_flags[d] == 1, jnp.flip(grid_data, axis=first_dim + d), grid_data)
    return grid_data

def fold_axis(grid_data, patch_axis, point_axis):
    extent = grid_data.shape[point_axis]
    first_plane = lax.slice_in_dim(grid_data, 0, 1, axis=point_axis)
    last_plane = lax.slice_in_dim(grid_data, extent - 1, extent, axis=point_axis)
    middle = lax.slice_in_dim(grid_data, 1, extent - 1, axis=point_axis)
    from_before = jnp.roll(last_plane, 1, axis=patch_axis)
    from_after = jnp.roll(first_plane, -1, axis=patch_axis)
    return jnp.concatenate([first_plane + from_before, middle, last_plane + from_after], axis=point_axis)

def reference(control_values, metric_diag, metric_off, mass_weight, orient):
    values_np, slopes_np = spline_tables(ELEMS)
    values = jnp.asarray(values_np)
    slopes = jnp.asarray(slopes_np)
    patches = N_PX * N_PY * N_PZ
    coeffs = control_values.reshape(N_PX, CTRL, N_PY, CTRL, N_PZ, CTRL, VECS)
    coeffs = coeffs.transpose(0, 2, 4, 1, 3, 5, 6).reshape(patches, CTRL, CTRL, CTRL, VECS)
    diag_all = metric_diag.reshape(3, N_PX, QUAD, N_PY, N_PZ, QUAD, QUAD)
    diag_all = diag_all.transpose(1, 3, 4, 0, 2, 5, 6).reshape(patches, 3, QUAD, QUAD, QUAD)
    off_all = metric_off.reshape(3, N_PX, QUAD, N_PY, N_PZ, QUAD, QUAD)
    off_all = off_all.transpose(1, 3, 4, 0, 2, 5, 6).reshape(patches, 3, QUAD, QUAD, QUAD)
    weight_all = mass_weight.reshape(N_PX, QUAD, N_PY, N_PZ, QUAD, QUAD)
    weight_all = weight_all.transpose(0, 2, 3, 1, 4, 5).reshape(patches, QUAD, QUAD, QUAD)
    flag_all = orient.reshape(patches, 3)

    def one_patch(patch_items):
        coeff_patch, diag_patch, off_patch, weight_patch, flag_patch = patch_items
        parts = forward_parts(coeff_patch, values, slopes)
        stiffness = stiffness_apply(parts, diag_patch, off_patch, values, slopes, QUAD)
        mass_part = mass_apply(parts[0], weight_patch, values, QUAD)
        return (flip_frame(stiffness, flag_patch, 0), flip_frame(mass_part, flag_patch, 0))
    stiffness_all, mass_all = lax.map(one_patch, (coeffs, diag_all, off_all, weight_all, flag_all))

    def assemble(grid_data):
        grid_data = grid_data.reshape(N_PX, N_PY, N_PZ, CTRL, CTRL, CTRL, VECS)
        grid_data = fold_axis(grid_data, 0, 3)
        grid_data = fold_axis(grid_data, 1, 4)
        grid_data = fold_axis(grid_data, 2, 5)
        return grid_data.reshape(patches, CTRL, CTRL, CTRL, VECS)

    def flip_back(patch_items):
        stiff_patch, mass_patch, flag_patch = patch_items
        return (flip_frame(stiff_patch, flag_patch, 0), flip_frame(mass_patch, flag_patch, 0))
    stiffness_all, mass_all = lax.map(flip_back, (assemble(stiffness_all), assemble(mass_all), flag_all))

    def to_layout(grid_data):
        grid_data = grid_data.reshape(N_PX, N_PY, N_PZ, CTRL, CTRL, CTRL, VECS)
        return grid_data.transpose(0, 3, 1, 4, 2, 5, 6).reshape(N_PX * CTRL, N_PY * CTRL, N_PZ * CTRL, VECS)
    return (to_layout(stiffness_all), to_layout(mass_all))
```

```python
import functools
import math

import jax
import jax.numpy as jnp
import numpy as np
from jax import lax
from jax.experimental import pallas as pl
from jax.experimental.pallas import tpu as pltpu
from jax.sharding import PartitionSpec as P

LANES = 128
ROWS = 8
F32 = jnp.float32
BF16 = jnp.bfloat16


def spline_tables(elements):
    knot_row = np.concatenate(
        [np.zeros(3), np.arange(elements + 1) * 1.0, np.full(3, float(elements))]
    )
    offsets = np.array([0.5 - 0.5 / math.sqrt(3.0), 0.5 + 0.5 / math.sqrt(3.0)])
    points = (np.arange(elements)[:, None] + offsets[None, :]).reshape(-1)
    intervals = np.repeat(np.arange(elements), 2) + 3
    current = np.zeros((points.size, knot_row.size - 1))
    current[np.arange(points.size), intervals] = 1.0
    previous = current
    for degree in range(1, 4):
        columns = knot_row.size - 1 - degree
        updated = np.zeros((points.size, columns))
        for i in range(columns):
            lower_gap = knot_row[i + degree] - knot_row[i]
            upper_gap = knot_row[i + degree + 1] - knot_row[i + 1]
            if lower_gap > 0:
                updated[:, i] += (points - knot_row[i]) / lower_gap * current[:, i]
            if upper_gap > 0:
                updated[:, i] += (knot_row[i + degree + 1] - points) / upper_gap * current[:, i + 1]
        previous = current
        current = updated
    slopes = np.zeros(current.shape)
    for i in range(current.shape[1]):
        lower_gap = knot_row[i + 3] - knot_row[i]
        upper_gap = knot_row[i + 4] - knot_row[i + 1]
        if lower_gap > 0:
            slopes[:, i] += 3.0 / lower_gap * previous[:, i]
        if upper_gap > 0:
            slopes[:, i] -= 3.0 / upper_gap * previous[:, i + 1]
    return (current.astype(np.float32), slopes.astype(np.float32))


def split(x):
    high = x.astype(BF16)
    return high, (x - high.astype(F32)).astype(BF16)


def split_np(x):
    high = x.astype(BF16)
    return high, (x - high.astype(np.float32)).astype(BF16)


def plane_tables(values, slopes):
    quad, ctrl = values.shape

    def pair(left, right):
        table = np.zeros((quad, quad, ROWS, ROWS), np.float32)
        table[:, :, :ctrl, :ctrl] = np.einsum("bj,ck->bcjk", left, right)
        return table.reshape(quad * quad, ROWS * ROWS)

    plain, by_y, by_z = pair(values, values), pair(slopes, values), pair(values, slopes)
    forward = np.concatenate([plain, by_y, by_z])
    high, low = split_np(forward)
    forward = np.concatenate([high, low, high], axis=1)
    zero = np.zeros_like(plain.T)
    back = np.concatenate(
        [
            np.concatenate([plain.T, by_y.T, by_z.T, zero], axis=1)[: ctrl * ROWS],
            np.concatenate([zero, zero, zero, plain.T], axis=1)[: ctrl * ROWS],
        ]
    )
    high, low = split_np(back)
    return forward, np.concatenate([high, low])


def forward_stage(u_ref, w_ref, p_ref, ctrl):
    vecs = u_ref.shape[-1]
    pad = jnp.zeros((ROWS - ctrl, vecs), F32)
    rest = jnp.zeros(((ROWS - ctrl) * ROWS, vecs), F32)
    for i in range(ctrl):
        rows = []
        for j in range(ctrl):
            rows += [u_ref[i, j], pad]
        high, low = split(jnp.concatenate(rows + [rest], axis=0))
        rhs = jnp.concatenate([high, high, low], axis=0)
        p_ref[i] = jnp.dot(w_ref[...], rhs, preferred_element_type=F32)


def metric_stage(diag_ref, off_ref, weight_ref, t_ref):
    quad = weight_ref.shape[0]
    for f in range(3):
        t_ref[f, :, 0:quad] = diag_ref[f].T
        t_ref[3 + f, :, 0:quad] = off_ref[f].T
    t_ref[6, :, 0:quad] = weight_ref[...].T


def point_stage(p_ref, t_ref, m_ref, h_ref, values, slopes, points, outs):
    quad, ctrl = values.shape
    vecs = p_ref.shape[-1]
    area = quad * quad

    def terms(column, table, index):
        total = None
        for i in range(ctrl):
            if table[index, i] != 0.0:
                term = float(table[index, i]) * column[i]
                total = term if total is None else total + term
        return total

    def body(b, carry):
        start = pl.multiple_of(b * quad, quad)
        for f in range(7):
            block = t_ref[f, pl.ds(start, quad), :]
            for a in points:
                m_ref[f * quad + a] = jnp.broadcast_to(block[:, a : a + 1], (quad, LANES))
        for lane in range(0, vecs, LANES):
            cols = pl.ds(lane, LANES)

            def loaded(kind):
                return {i: p_ref[i, pl.ds(pl.multiple_of(kind * area + start, quad), quad), cols] for i in range(ctrl)}

            plain, by_y, by_z = loaded(0), loaded(1), loaded(2)
            sums = [[None] * 4 for _ in outs]

            def gather(n, field, factor, value):
                if factor != 0.0:
                    term = float(factor) * value
                    old = sums[n][field]
                    sums[n][field] = term if old is None else old + term

            for a in points:
                d0, d1, d2, o0, o1, o2, w = (m_ref[f * quad + a] for f in range(7))
                gx = terms(plain, slopes, a)
                gy = terms(by_y, values, a)
                gz = terms(by_z, values, a)
                gp = terms(plain, values, a)
                fx = d0 * gx + o0 * gy + o1 * gz
                fy = o0 * gx + d1 * gy + o2 * gz
                fz = o1 * gx + o2 * gy + d2 * gz
                fm = w * gp
                for n, i in enumerate(outs):
                    gather(n, 0, slopes[a, i], fx)
                    gather(n, 1, values[a, i], fy)
                    gather(n, 2, values[a, i], fz)
                    gather(n, 3, values[a, i], fm)
            for n in range(len(outs)):
                for field in range(4):
                    rows = pl.ds(pl.multiple_of(field * area + start, quad), quad)
                    h_ref[n, rows, cols] = sums[n][field]
        return carry

    lax.fori_loop(0, quad, body, 0)


def back_plane(h, w_ref):
    half = w_ref.shape[0] // 2
    high, low = split(h)
    both = jnp.dot(w_ref[...], high, preferred_element_type=F32)
    return both[:half] + both[half:] + jnp.dot(w_ref[0:half], low, preferred_element_type=F32)


def turned(x, flag, ctrl):
    rows = lax.broadcasted_iota(jnp.int32, x.shape, 0)
    back = jnp.where(rows < ctrl, ctrl - 1 - rows, rows)
    return jnp.take_along_axis(x, jnp.where(flag == 1, back, rows), axis=0, mode="promise_in_bounds")


def at(index, flag, ctrl):
    return jnp.where(flag == 1, ctrl - 1 - index, index)


def edge_kernel(values, slopes, flags, u_ref, diag_ref, off_ref, weight_ref, wf_ref, wb_ref, low_ref, high_ref,
                p_ref, t_ref, m_ref, h_ref, o_ref):
    quad, ctrl = values.shape
    metric_stage(diag_ref, off_ref, weight_ref, t_ref)
    forward_stage(u_ref, wf_ref, p_ref, ctrl)
    ends = (0, ctrl - 1)
    points = [a for a in range(quad) if values[a, 0] != 0.0 or values[a, ctrl - 1] != 0.0]
    point_stage(p_ref, t_ref, m_ref, h_ref, values, slopes, points, ends)
    fi, fj, fk = flags[0], flags[1], flags[2]
    for n in range(2):
        o_ref[n] = back_plane(h_ref[n], wb_ref)
    area = ctrl * ROWS
    for side, out_ref in ((0, low_ref), (1, high_ref)):
        which = jnp.where(fi == 1, 1 - side, side)
        for field in range(2):
            for j in range(ctrl):
                start = pl.multiple_of(field * area + at(j, fj, ctrl) * ROWS, ROWS)
                out_ref[field, j] = turned(o_ref[which, pl.ds(start, ROWS), :], fk, ctrl)[0:ctrl]


def body_kernel(values, slopes, u_ref, diag_ref, off_ref, weight_ref, wf_ref, wb_ref, out_ref,
                p_ref, t_ref, m_ref, h_ref):
    quad, ctrl = values.shape
    metric_stage(diag_ref, off_ref, weight_ref, t_ref)
    forward_stage(u_ref, wf_ref, p_ref, ctrl)
    point_stage(p_ref, t_ref, m_ref, h_ref, values, slopes, range(quad), range(ctrl))
    area = ctrl * ROWS
    for i in range(ctrl):
        both = back_plane(h_ref[i], wb_ref)
        for lane in range(out_ref.shape[2]):
            part = both[:, lane * LANES : (lane + 1) * LANES]
            out_ref[0, i, lane] = part[:area]
            out_ref[1, i, lane] = part[area:]


def pack_kernel(ctrl, flags, bulk_ref, xlow_ref, xhigh_ref, y_ref, zlow_ref, zhigh_ref, dlow_ref, dhigh_ref):
    fi, fj, fk = flags[0], flags[1], flags[2]
    last = ctrl - 1
    pad = jnp.zeros((ROWS - ctrl, LANES), F32)
    for field, i, lane in np.ndindex(2, ctrl, bulk_ref.shape[2]):
        here = at(i, fi, ctrl)
        cols = pl.ds(lane * LANES, LANES)
        x_ref = xlow_ref if i == 0 else xhigh_ref if i == last else None
        for side, j in ((0, 0), (1, last)):
            start = pl.multiple_of(at(j, fj, ctrl) * ROWS, ROWS)
            block = turned(bulk_ref[field, here, lane, pl.ds(start, ROWS), :], fk, ctrl)[0:ctrl]
            if x_ref is not None:
                block = block + x_ref[field, j, :, cols]
            y_ref[side, field, i, :, cols] = block
        for k, z_ref, d_ref in ((0, zlow_ref, dlow_ref), (last, zhigh_ref, dhigh_ref)):
            block = bulk_ref[field, here, lane, pl.ds(at(k, fk, ctrl), ctrl, stride=ROWS), :]
            block = turned(jnp.concatenate([block, pad], axis=0), fj, ctrl)[0:ctrl]
            if x_ref is not None:
                block = block + jnp.concatenate([x_ref[field, j, k : k + 1, cols] for j in range(ctrl)], axis=0)
            z_ref[field, i, :, cols] = block
            for end, j in ((0, 0), (1, last)):
                d_ref[end, field, i : i + 1, cols] = block[j : j + 1]


def join_kernel(ctrl, flags, bulk_ref, xlow_ref, xhigh_ref, y_ref, zlow_ref, zhigh_ref, dlow_ref, dhigh_ref,
                k_ref, n_ref):
    fi, fj, fk = flags[0], flags[1], flags[2]
    last = ctrl - 1
    rows = lax.broadcasted_iota(jnp.int32, (ROWS, LANES), 0)
    at_low, at_high = rows == at(0, fk, ctrl), rows == at(last, fk, ctrl)
    pad = jnp.zeros((ROWS - ctrl, LANES), F32)

    def spread(row):
        return jnp.broadcast_to(row, (ROWS, LANES))

    def arrived(block):
        return turned(jnp.concatenate([block, pad], axis=0), fk, ctrl)

    for field, i, j, lane in np.ndindex(2, ctrl, ctrl, bulk_ref.shape[2]):
        out_ref = (k_ref, n_ref)[field]
        cols = pl.ds(lane * LANES, LANES)
        here, there = at(i, fi, ctrl), at(j, fj, ctrl)
        x_ref = xlow_ref if i == 0 else xhigh_ref if i == last else None
        rim = 1 if j == 0 else 0 if j == last else None
        block = bulk_ref[field, here, lane, pl.ds(pl.multiple_of(there * ROWS, ROWS), ROWS), :]
        extra = None
        if x_ref is not None:
            extra = x_ref[field, j, :, cols]
        if rim is not None:
            more = y_ref[rim, field, i, :, cols]
            extra = more if extra is None else extra + more
        if extra is not None:
            block = block + arrived(extra)
        low, high = zlow_ref[field, i, j : j + 1, cols], zhigh_ref[field, i, j : j + 1, cols]
        if rim is not None:
            low = low + dlow_ref[rim, field, i : i + 1, cols]
            high = high + dhigh_ref[rim, field, i : i + 1, cols]
        block = block + jnp.where(at_low, spread(low), jnp.where(at_high, spread(high), 0.0))
        out_ref[here, there, :, cols] = block[0:ctrl]


def shifted(x, axes, sizes, steps):
    pairs = []
    for index in np.ndindex(*sizes):
        to = [(p + s) % n for p, s, n in zip(index, steps, sizes)]
        pairs.append((int(np.ravel_multi_index(index, sizes)), int(np.ravel_multi_index(to, sizes))))
    return lax.ppermute(x, axes, pairs)


def per_device(sizes, control_values, metric_diag, metric_off, mass_weight, orient):
    quad = mass_weight.shape[0]
    ctrl, vecs = control_values.shape[0], control_values.shape[-1]
    values, slopes = spline_tables(quad // 2)
    wf_np, wb_np = plane_tables(values, slopes)
    wf, wb = jnp.asarray(wf_np), jnp.asarray(wb_np)
    flags = orient.reshape(3)
    vmem = pl.BlockSpec(memory_space=pltpu.VMEM)
    smem = pl.BlockSpec(memory_space=pltpu.SMEM)
    area = quad * quad
    nx, ny, nz = sizes

    def scratch(planes):
        return [
            pltpu.VMEM((ctrl, 3 * area, vecs), F32),
            pltpu.VMEM((7, area, LANES), F32),
            pltpu.VMEM((7 * quad, quad, LANES), F32),
            pltpu.VMEM((planes, 4 * area, vecs), F32),
        ]

    def sd(*shape):
        return jax.ShapeDtypeStruct(shape, F32)

    fields = (metric_diag, metric_off, mass_weight, wf, wb)
    xlow, xhigh = pl.pallas_call(
        functools.partial(edge_kernel, values, slopes),
        out_shape=[sd(2, ctrl, ctrl, vecs)] * 2,
        in_specs=[smem] + [vmem] * 6,
        out_specs=[vmem] * 2,
        scratch_shapes=scratch(2) + [pltpu.VMEM((2, 2 * ctrl * ROWS, vecs), F32)],
        cost_estimate=pl.CostEstimate(flops=10**9, bytes_accessed=10**6, transcendentals=0),
        compiler_params=pltpu.CompilerParams(vmem_limit_bytes=12 * 2**20),
        name="edge",
    )(flags, control_values, *fields)
    from_low = shifted(xhigh, ("px",), (nx,), (1,))
    from_high = shifted(xlow, ("px",), (nx,), (-1,))
    bulk = pl.pallas_call(
        functools.partial(body_kernel, values, slopes),
        out_shape=sd(2, ctrl, vecs // LANES, ctrl * ROWS, LANES),
        in_specs=[vmem] * 6,
        out_specs=vmem,
        scratch_shapes=scratch(ctrl),
        cost_estimate=pl.CostEstimate(flops=2 * 10**9, bytes_accessed=10**6, transcendentals=0),
        compiler_params=pltpu.CompilerParams(vmem_limit_bytes=16 * 2**20),
        name="body",
    )(control_values, *fields)
    ysend, zlow, zhigh, dlow, dhigh = pl.pallas_call(
        functools.partial(pack_kernel, ctrl),
        out_shape=[sd(2, 2, ctrl, ctrl, vecs)] + [sd(2, ctrl, ctrl, vecs)] * 2 + [sd(2, 2, ctrl, vecs)] * 2,
        in_specs=[smem] + [vmem] * 3,
        out_specs=[vmem] * 5,
        cost_estimate=pl.CostEstimate(flops=10**7, bytes_accessed=10**6, transcendentals=0),
        compiler_params=pltpu.CompilerParams(vmem_limit_bytes=8 * 2**20),
        name="pack",
    )(flags, bulk, from_low, from_high)
    yz, yzn = ("py", "pz"), (ny, nz)

    def crossed(pair, axes, counts, *steps):
        if ny == 2:
            return shifted(pair, axes, counts, (1, *steps))
        return jnp.stack([shifted(pair[0], axes, counts, (-1, *steps)), shifted(pair[1], axes, counts, (1, *steps))])

    dlow_in = crossed(dhigh, yz, yzn, 1)
    dhigh_in = crossed(dlow, yz, yzn, -1)
    y_in = crossed(ysend, ("py",), (ny,))
    zlow_in = shifted(zhigh, ("pz",), (nz,), (1,))
    zhigh_in = shifted(zlow, ("pz",), (nz,), (-1,))
    return tuple(
        pl.pallas_call(
            functools.partial(join_kernel, ctrl),
            out_shape=[sd(ctrl, ctrl, ctrl, vecs)] * 2,
            in_specs=[smem] + [vmem] * 8,
            out_specs=[vmem] * 2,
            cost_estimate=pl.CostEstimate(flops=10**7, bytes_accessed=10**6, transcendentals=0),
            compiler_params=pltpu.CompilerParams(vmem_limit_bytes=10 * 2**20),
        name="join",
        )(flags, bulk, from_low, from_high, y_in, zlow_in, zhigh_in, dlow_in, dhigh_in)
    )


def solution(mesh):
    in_specs = (
        P("px", "py", "pz", None),
        P(None, "px", ("py", "pz")),
        P(None, "px", ("py", "pz")),
        P("px", ("py", "pz")),
        P("px", "py", "pz", None),
    )
    out_specs = (P("px", "py", "pz", None), P("px", "py", "pz", None))
    sizes = (mesh.shape["px"], mesh.shape["py"], mesh.shape["pz"])
    return jax.shard_map(
        functools.partial(per_device, sizes), mesh=mesh, in_specs=in_specs, out_specs=out_specs, check_vma=False
    )
```

```python
import functools
import itertools
import math

import jax
import jax.numpy as jnp
import numpy as np
from jax import lax
from jax.experimental import pallas as pl
from jax.experimental.pallas import tpu as pltpu
from jax.sharding import PartitionSpec as P


LANES = 128
ROWS = 8
F32 = jnp.float32
BF16 = jnp.bfloat16


def spline_tables(elements):
    knot_row = np.concatenate(
        [np.zeros(3), np.arange(elements + 1) * 1.0, np.full(3, float(elements))]
    )
    offsets = np.array([0.5 - 0.5 / math.sqrt(3.0), 0.5 + 0.5 / math.sqrt(3.0)])
    points = (np.arange(elements)[:, None] + offsets[None, :]).reshape(-1)
    intervals = np.repeat(np.arange(elements), 2) + 3
    current = np.zeros((points.size, knot_row.size - 1))
    current[np.arange(points.size), intervals] = 1.0
    previous = current
    for degree in range(1, 4):
        columns = knot_row.size - 1 - degree
        updated = np.zeros((points.size, columns))
        for i in range(columns):
            lower_gap = knot_row[i + degree] - knot_row[i]
            upper_gap = knot_row[i + degree + 1] - knot_row[i + 1]
            if lower_gap > 0:
                updated[:, i] += (points - knot_row[i]) / lower_gap * current[:, i]
            if upper_gap > 0:
                updated[:, i] += (knot_row[i + degree + 1] - points) / upper_gap * current[:, i + 1]
        previous = current
        current = updated
    slopes = np.zeros(current.shape)
    for i in range(current.shape[1]):
        lower_gap = knot_row[i + 3] - knot_row[i]
        upper_gap = knot_row[i + 4] - knot_row[i + 1]
        if lower_gap > 0:
            slopes[:, i] += 3.0 / lower_gap * previous[:, i]
        if upper_gap > 0:
            slopes[:, i] -= 3.0 / upper_gap * previous[:, i + 1]
    return (current.astype(np.float32), slopes.astype(np.float32))


def split(x):
    high = x.astype(BF16)
    return high, (x - high.astype(F32)).astype(BF16)


def split_np(x):
    high = x.astype(BF16)
    return high, (x - high.astype(np.float32)).astype(BF16)


def plane_tables(values, slopes):
    quad, ctrl = values.shape

    def pair(left, right):
        table = np.zeros((quad, quad, ROWS, ROWS), np.float32)
        table[:, :, :ctrl, :ctrl] = np.einsum("bj,ck->bcjk", left, right)
        return table.reshape(quad * quad, ROWS * ROWS)

    plain, by_y, by_z = pair(values, values), pair(slopes, values), pair(values, slopes)
    forward = np.concatenate([plain, by_y, by_z])
    high, low = split_np(forward)
    forward = np.concatenate([high, low, high], axis=1)
    zero = np.zeros_like(plain.T)
    back = np.concatenate(
        [
            np.concatenate([plain.T, by_y.T, by_z.T, zero], axis=1)[: ctrl * ROWS],
            np.concatenate([zero, zero, zero, plain.T], axis=1)[: ctrl * ROWS],
        ]
    )
    high, low = split_np(back)
    return forward, np.concatenate([high, low])


def forward_stage(u_ref, w_ref, p_ref, ctrl, arrive):
    vecs = u_ref.shape[-1]
    pad = jnp.zeros((ROWS - ctrl, vecs), F32)
    rest = jnp.zeros(((ROWS - ctrl) * ROWS, vecs), F32)
    for i in range(ctrl):
        arrive(i)
        rows = []
        for j in range(ctrl):
            rows += [u_ref[i, j], pad]
        high, low = split(jnp.concatenate(rows + [rest], axis=0))
        rhs = jnp.concatenate([high, high, low], axis=0)
        p_ref[i] = jnp.dot(w_ref[...], rhs, preferred_element_type=F32)


def metric_stage(diag_ref, off_ref, weight_ref, t_ref):
    quad = weight_ref.shape[0]
    for f in range(3):
        t_ref[f, :, 0:quad] = diag_ref[f].T
        t_ref[3 + f, :, 0:quad] = off_ref[f].T
    t_ref[6, :, 0:quad] = weight_ref[...].T


def point_stage(p_ref, t_ref, m_ref, h_ref, values, slopes, points, outs):
    quad, ctrl = values.shape
    vecs = p_ref.shape[-1]
    area = quad * quad

    def terms(column, table, index):
        total = None
        for i in range(ctrl):
            if table[index, i] != 0.0:
                term = float(table[index, i]) * column[i]
                total = term if total is None else total + term
        return total

    def body(b, carry):
        start = pl.multiple_of(b * quad, quad)
        for f in range(7):
            block = t_ref[f, pl.ds(start, quad), :]
            for a in points:
                m_ref[f * quad + a] = jnp.broadcast_to(block[:, a : a + 1], (quad, LANES))
        for lane in range(0, vecs, LANES):
            cols = pl.ds(lane, LANES)

            def loaded(kind):
                return {i: p_ref[i, pl.ds(pl.multiple_of(kind * area + start, quad), quad), cols] for i in range(ctrl)}

            plain, by_y, by_z = loaded(0), loaded(1), loaded(2)
            sums = [[None] * 4 for _ in outs]

            def gather(n, field, factor, value):
                if factor != 0.0:
                    term = float(factor) * value
                    old = sums[n][field]
                    sums[n][field] = term if old is None else old + term

            for a in points:
                d0, d1, d2, o0, o1, o2, w = (m_ref[f * quad + a] for f in range(7))
                gx = terms(plain, slopes, a)
                gy = terms(by_y, values, a)
                gz = terms(by_z, values, a)
                gp = terms(plain, values, a)
                fx = d0 * gx + o0 * gy + o1 * gz
                fy = o0 * gx + d1 * gy + o2 * gz
                fz = o1 * gx + o2 * gy + d2 * gz
                fm = w * gp
                for n, i in enumerate(outs):
                    gather(n, 0, slopes[a, i], fx)
                    gather(n, 1, values[a, i], fy)
                    gather(n, 2, values[a, i], fz)
                    gather(n, 3, values[a, i], fm)
            for n in range(len(outs)):
                for field in range(4):
                    rows = pl.ds(pl.multiple_of(field * area + start, quad), quad)
                    h_ref[n, rows, cols] = sums[n][field]
        return carry

    lax.fori_loop(0, quad, body, 0)


def back_plane(h, w_ref):
    half = w_ref.shape[0] // 2
    high, low = split(h)
    both = jnp.dot(w_ref[...], high, preferred_element_type=F32)
    return both[:half] + both[half:] + jnp.dot(w_ref[0:half], low, preferred_element_type=F32)


def turned(x, flag, ctrl):
    rows = lax.broadcasted_iota(jnp.int32, x.shape, 0)
    back = jnp.where(rows < ctrl, ctrl - 1 - rows, rows)
    return jnp.take_along_axis(x, jnp.where(flag == 1, back, rows), axis=0, mode="promise_in_bounds")


def at(index, flag, ctrl):
    return jnp.where(flag == 1, ctrl - 1 - index, index)


def body_kernel(values, slopes, flags_in, u_in, diag_in, off_in, weight_in, wf_in, wb_in,
                bulk_ref, xlow_ref, xhigh_ref, dlow_ref, dhigh_ref,
                flags, u_ref, diag_ref, off_ref, weight_ref, wf_ref, wb_ref, u_sems, sems, p_ref, t_ref, m_ref, h_ref):
    quad, ctrl = values.shape
    last = ctrl - 1
    small = [
        pltpu.make_async_copy(src, dst, sems.at[n])
        for n, (src, dst) in enumerate(
            ((wf_in, wf_ref), (diag_in, diag_ref), (off_in, off_ref), (weight_in, weight_ref), (wb_in, wb_ref), (flags_in, flags))
        )
    ]
    planes = [pltpu.make_async_copy(u_in.at[i], u_ref.at[i], u_sems.at[i]) for i in range(ctrl)]
    for copy in small[:1] + planes + small[1:]:
        copy.start()
    small[0].wait()
    forward_stage(u_ref, wf_ref, p_ref, ctrl, lambda i: planes[i].wait())
    for copy in small[1:]:
        copy.wait()
    metric_stage(diag_ref, off_ref, weight_ref, t_ref)
    point_stage(p_ref, t_ref, m_ref, h_ref, values, slopes, range(quad), range(ctrl))
    area = ctrl * ROWS
    lanes = bulk_ref.shape[2]
    for i in range(ctrl):
        both = back_plane(h_ref[i], wb_ref)
        for lane in range(lanes):
            part = both[:, lane * LANES : (lane + 1) * LANES]
            bulk_ref[0, i, lane] = part[:area]
            bulk_ref[1, i, lane] = part[area:]
    fi, fj, fk = flags[0], flags[1], flags[2]
    for field, lane in np.ndindex(2, lanes):
        cols = pl.ds(lane * LANES, LANES)
        for i, x_ref in ((0, xlow_ref), (last, xhigh_ref)):
            here = at(i, fi, ctrl)
            for line, j in ((0, 0), (1, last)):
                x_ref[pl.ds((line * 2 + field) * ctrl, ctrl), cols] = y_line(bulk_ref, field, here, lane, j, flags, ctrl)
            for line, k in ((2, 0), (3, last)):
                x_ref[pl.ds((line * 2 + field) * ctrl, ctrl), cols] = z_line(bulk_ref, field, here, lane, k, flags, ctrl)
        for i, (side, j), (k, d_ref) in itertools.product(range(ctrl), ((0, 0), (1, last)), ((0, dlow_ref), (last, dhigh_ref))):
            row = at(j, fj, ctrl) * ROWS + at(k, fk, ctrl)
            d_ref[pl.ds((side * 2 + field) * ctrl + i, 1), cols] = bulk_ref[field, at(i, fi, ctrl), lane, pl.ds(row, 1), :]


def y_line(bulk_ref, field, here, lane, j, flags, ctrl):
    start = pl.multiple_of(at(j, flags[1], ctrl) * ROWS, ROWS)
    return turned(bulk_ref[field, here, lane, pl.ds(start, ROWS), :], flags[2], ctrl)[0:ctrl]


def z_line(bulk_ref, field, here, lane, k, flags, ctrl):
    block = bulk_ref[field, here, lane, pl.ds(at(k, flags[2], ctrl), ctrl, stride=ROWS), :]
    pad = jnp.zeros((ROWS - ctrl, LANES), F32)
    return turned(jnp.concatenate([block, pad], axis=0), flags[1], ctrl)[0:ctrl]


def pack_kernel(ctrl, flags, bulk_ref, xlow_ref, xhigh_ref, y_ref, zlow_ref, zhigh_ref):
    last = ctrl - 1
    for field, i, lane in np.ndindex(2, ctrl, bulk_ref.shape[2]):
        here = at(i, flags[0], ctrl)
        cols = pl.ds(lane * LANES, LANES)
        x_ref = xlow_ref if i == 0 else xhigh_ref if i == last else None

        def summed(block, line):
            return block if x_ref is None else block + x_ref[pl.ds((line * 2 + field) * ctrl, ctrl), cols]

        for side, j in ((0, 0), (1, last)):
            block = y_line(bulk_ref, field, here, lane, j, flags, ctrl)
            y_ref[pl.ds(((side * 2 + field) * ctrl + i) * ctrl, ctrl), cols] = summed(block, side)
        for side, k, z_ref in ((0, 0, zlow_ref), (1, last, zhigh_ref)):
            block = z_line(bulk_ref, field, here, lane, k, flags, ctrl)
            z_ref[pl.ds((field * ctrl + i) * ctrl, ctrl), cols] = summed(block, 2 + side)


def late_kernel(ctrl, flags, bulk_ref, dlow_ref, dhigh_ref, low_ref, high_ref):
    last = ctrl - 1
    inner = ctrl - 2
    for i, out_ref in ((0, low_ref), (last, high_ref)):
        here = at(i, flags[0], ctrl)
        for field, lane in np.ndindex(2, bulk_ref.shape[2]):
            cols = pl.ds(lane * LANES, LANES)
            for j in range(1, last):
                block = y_line(bulk_ref, field, here, lane, j, flags, ctrl)
                out_ref[pl.ds((field * inner + j - 1) * ctrl, ctrl), cols] = block
        for end, d_ref in enumerate((dlow_ref, dhigh_ref)):
            for side, field in np.ndindex(2, 2):
                row = 2 * inner * ctrl + (end * 2 + side) * 2 + field
                out_ref[pl.ds(row, 1), :] = d_ref[pl.ds((side * 2 + field) * ctrl + i, 1), :]


def join_kernel(ctrl, flags, bulk_ref, xlow_ref, xhigh_ref, llow_ref, lhigh_ref, y_ref, zlow_ref, zhigh_ref,
                dlow_ref, dhigh_ref, k_out, n_out, stage_ref, sems):
    fi, fj, fk = flags[0], flags[1], flags[2]
    last = ctrl - 1
    inner = ctrl - 2
    rows = lax.broadcasted_iota(jnp.int32, (ROWS, LANES), 0)
    at_low, at_high = rows == at(0, fk, ctrl), rows == at(last, fk, ctrl)
    pad = jnp.zeros((ROWS - ctrl, LANES), F32)
    copies = []

    def spread(row):
        return jnp.broadcast_to(row, (ROWS, LANES))

    for i, field in np.ndindex(ctrl, 2):
        here = at(i, fi, ctrl)
        x_ref, l_ref = (xlow_ref, llow_ref) if i == 0 else (xhigh_ref, lhigh_ref) if i == last else (None, None)
        for j, lane in np.ndindex(ctrl, bulk_ref.shape[2]):
            cols = pl.ds(lane * LANES, LANES)
            there = at(j, fj, ctrl)
            rim = 1 if j == 0 else 0 if j == last else None
            block = bulk_ref[field, here, lane, pl.ds(pl.multiple_of(there * ROWS, ROWS), ROWS), :]
            extra = []
            if x_ref is not None:
                if rim is None:
                    extra.append(l_ref[pl.ds((field * inner + j - 1) * ctrl, ctrl), cols])
                else:
                    extra.append(x_ref[pl.ds(((1 - rim) * 2 + field) * ctrl, ctrl), cols])
            if rim is not None:
                extra.append(y_ref[pl.ds(((rim * 2 + field) * ctrl + i) * ctrl, ctrl), cols])
            if extra:
                block = block + turned(jnp.concatenate([sum(extra[1:], extra[0]), pad], axis=0), fk, ctrl)
            ends = []
            for end, (z_ref, d_ref) in enumerate(((zlow_ref, dlow_ref), (zhigh_ref, dhigh_ref))):
                row = z_ref[pl.ds((field * ctrl + i) * ctrl + j, 1), cols]
                if rim is not None:
                    row = row + d_ref[pl.ds((rim * 2 + field) * ctrl + i, 1), cols]
                    if l_ref is not None:
                        row = row + l_ref[pl.ds(2 * inner * ctrl + (end * 2 + rim) * 2 + field, 1), cols]
                ends.append(spread(row))
            block = block + jnp.where(at_low, ends[0], jnp.where(at_high, ends[1], 0.0))
            stage_ref[field, i, there, :, cols] = block[0:ctrl]
        copy = pltpu.make_async_copy(stage_ref.at[field, i], (k_out, n_out)[field].at[here], sems.at[field, i])
        copy.start()
        copies.append(copy)
    for copy in copies:
        copy.wait()


def shifted(x, axes, sizes, steps):
    pairs = []
    for index in np.ndindex(*sizes):
        to = [(p + s) % n for p, s, n in zip(index, steps, sizes)]
        pairs.append((int(np.ravel_multi_index(index, sizes)), int(np.ravel_multi_index(to, sizes))))
    return lax.ppermute(x, axes, pairs)


def per_device(sizes, control_values, metric_diag, metric_off, mass_weight, orient):
    quad = mass_weight.shape[0]
    ctrl, vecs = control_values.shape[0], control_values.shape[-1]
    values, slopes = spline_tables(quad // 2)
    wf_np, wb_np = plane_tables(values, slopes)
    wf, wb = jnp.asarray(wf_np), jnp.asarray(wb_np)
    flags = orient.reshape(3)
    hbm = pl.BlockSpec(memory_space=pltpu.HBM)
    vmem = pl.BlockSpec(memory_space=pltpu.VMEM)
    smem = pl.BlockSpec(memory_space=pltpu.SMEM)
    area = quad * quad
    nx, ny, nz = sizes
    face = 2 * ctrl * ctrl

    def sd(*shape):
        return jax.ShapeDtypeStruct(shape, F32)

    def call(kernel, mib, flops, **kwargs):
        def run(*args):
            return pl.pallas_call(
                kernel,
                compiler_params=pltpu.CompilerParams(vmem_limit_bytes=mib * 2**20),
                cost_estimate=pl.CostEstimate(flops=flops, bytes_accessed=10**6, transcendentals=0),
                **kwargs,
            )(*args)

        return run

    def crossed(pair, axes, counts, *steps):
        if ny == 2:
            return shifted(pair, axes, counts, (1, *steps))
        half = pair.shape[0] // 2
        return jnp.concatenate(
            [shifted(pair[:half], axes, counts, (-1, *steps)), shifted(pair[half:], axes, counts, (1, *steps))]
        )

    yz, yzn = ("py", "pz"), (ny, nz)
    inputs = (flags, control_values, metric_diag, metric_off, mass_weight, wf, wb)
    bulk, xlow, xhigh, dlow, dhigh = call(
        functools.partial(body_kernel, values, slopes),
        20,
        10**9,
        out_shape=[sd(2, ctrl, vecs // LANES, ctrl * ROWS, LANES)] + [sd(8 * ctrl, vecs)] * 2 + [sd(4 * ctrl, vecs)] * 2,
        in_specs=[hbm] * 7,
        out_specs=[vmem] * 5,
        scratch_shapes=[
            pltpu.SMEM((3,), jnp.int32),
            pltpu.VMEM(control_values.shape, F32),
            pltpu.VMEM(metric_diag.shape, F32),
            pltpu.VMEM(metric_off.shape, F32),
            pltpu.VMEM(mass_weight.shape, F32),
            pltpu.VMEM(wf.shape, BF16),
            pltpu.VMEM(wb.shape, BF16),
            pltpu.SemaphoreType.DMA((ctrl,)),
            pltpu.SemaphoreType.DMA((6,)),
            pltpu.VMEM((ctrl, 3 * area, vecs), F32),
            pltpu.VMEM((7, area, LANES), F32),
            pltpu.VMEM((7 * quad, quad, LANES), F32),
            pltpu.VMEM((ctrl, 4 * area, vecs), F32),
        ],
    )(*(pltpu.with_memory_space_constraint(x, pltpu.HBM) for x in inputs))
    xlow_in = shifted(xhigh, ("px",), (nx,), (1,))
    xhigh_in = shifted(xlow, ("px",), (nx,), (-1,))
    dlow_in = crossed(dhigh, yz, yzn, 1)
    dhigh_in = crossed(dlow, yz, yzn, -1)
    ysend, zlow, zhigh = call(
        functools.partial(pack_kernel, ctrl),
        8,
        10**8,
        out_shape=[sd(2 * face, vecs)] + [sd(face, vecs)] * 2,
        in_specs=[smem] + [vmem] * 3,
        out_specs=[vmem] * 3,
    )(flags, bulk, xlow_in, xhigh_in)
    zlow_in = shifted(zhigh, ("pz",), (nz,), (1,))
    y_in = crossed(ysend, ("py",), (ny,))
    zhigh_in = shifted(zlow, ("pz",), (nz,), (-1,))
    late = 2 * (ctrl - 2) * ctrl + 8
    llow, lhigh = call(
        functools.partial(late_kernel, ctrl),
        8,
        10**7,
        out_shape=[sd(late, vecs)] * 2,
        in_specs=[smem] + [vmem] * 3,
        out_specs=[vmem] * 2,
    )(flags, bulk, dlow_in, dhigh_in)
    llow_in = shifted(lhigh, ("px",), (nx,), (1,))
    lhigh_in = shifted(llow, ("px",), (nx,), (-1,))
    return tuple(
        call(
            functools.partial(join_kernel, ctrl),
            10,
            10**8,
            out_shape=[sd(*control_values.shape)] * 2,
            in_specs=[smem] + [vmem] * 10,
            out_specs=[hbm] * 2,
            scratch_shapes=[pltpu.VMEM((2, *control_values.shape), F32), pltpu.SemaphoreType.DMA((2, ctrl))],
        )(flags, bulk, xlow_in, xhigh_in, llow_in, lhigh_in, y_in, zlow_in, zhigh_in, dlow_in, dhigh_in)
    )


def solution(mesh):
    in_specs = (
        P("px", "py", "pz", None),
        P(None, "px", ("py", "pz")),
        P(None, "px", ("py", "pz")),
        P("px", ("py", "pz")),
        P("px", "py", "pz", None),
    )
    out_specs = (P("px", "py", "pz", None), P("px", "py", "pz", None))
    sizes = (mesh.shape["px"], mesh.shape["py"], mesh.shape["pz"])

    def body(*args):
        return per_device(sizes, *args)

    return jax.shard_map(body, mesh=mesh, in_specs=in_specs, out_specs=out_specs, check_vma=False)
```

```python
import functools
import itertools
import math

import jax
import jax.numpy as jnp
import numpy as np
from jax import lax
from jax.experimental import pallas as pl
from jax.experimental.pallas import tpu as pltpu
from jax.sharding import PartitionSpec as P


LANES = 128
ROWS = 8
F32 = jnp.float32
BF16 = jnp.bfloat16


def spline_tables(elements):
    knot_row = np.concatenate(
        [np.zeros(3), np.arange(elements + 1) * 1.0, np.full(3, float(elements))]
    )
    offsets = np.array([0.5 - 0.5 / math.sqrt(3.0), 0.5 + 0.5 / math.sqrt(3.0)])
    points = (np.arange(elements)[:, None] + offsets[None, :]).reshape(-1)
    intervals = np.repeat(np.arange(elements), 2) + 3
    current = np.zeros((points.size, knot_row.size - 1))
    current[np.arange(points.size), intervals] = 1.0
    previous = current
    for degree in range(1, 4):
        columns = knot_row.size - 1 - degree
        updated = np.zeros((points.size, columns))
        for i in range(columns):
            lower_gap = knot_row[i + degree] - knot_row[i]
            upper_gap = knot_row[i + degree + 1] - knot_row[i + 1]
            if lower_gap > 0:
                updated[:, i] += (points - knot_row[i]) / lower_gap * current[:, i]
            if upper_gap > 0:
                updated[:, i] += (knot_row[i + degree + 1] - points) / upper_gap * current[:, i + 1]
        previous = current
        current = updated
    slopes = np.zeros(current.shape)
    for i in range(current.shape[1]):
        lower_gap = knot_row[i + 3] - knot_row[i]
        upper_gap = knot_row[i + 4] - knot_row[i + 1]
        if lower_gap > 0:
            slopes[:, i] += 3.0 / lower_gap * previous[:, i]
        if upper_gap > 0:
            slopes[:, i] -= 3.0 / upper_gap * previous[:, i + 1]
    return (current.astype(np.float32), slopes.astype(np.float32))


def split(x):
    high = x.astype(BF16)
    return high, (x - high.astype(F32)).astype(BF16)


def split_np(x):
    high = x.astype(BF16)
    return high, (x - high.astype(np.float32)).astype(BF16)


def plane_tables(values, slopes):
    quad, ctrl = values.shape

    def pair(left, right):
        table = np.zeros((quad, quad, ROWS, ROWS), np.float32)
        table[:, :, :ctrl, :ctrl] = np.einsum("bj,ck->bcjk", left, right)
        return table.reshape(quad * quad, ROWS * ROWS)

    plain, by_y, by_z = pair(values, values), pair(slopes, values), pair(values, slopes)
    high, low = split_np(np.concatenate([plain, by_y, by_z]))
    forward = np.concatenate([high, low, high], axis=1)
    zero = np.zeros_like(plain.T)
    used = ctrl * ROWS
    back = np.concatenate(
        [
            np.concatenate([plain.T, zero, zero, zero], axis=1)[:used],
            np.concatenate([zero, by_y.T, by_z.T, zero], axis=1)[:used],
            np.concatenate([zero, zero, zero, plain.T], axis=1)[:used],
        ]
    )
    high, low = split_np(back)
    return forward, np.concatenate([high, low, high], axis=1)


def terms(table, index, column):
    total = None
    for n in range(table.shape[1]):
        if table[index, n] != 0.0:
            term = float(table[index, n]) * column(n)
            total = term if total is None else total + term
    return total


def operand_stage(a, u_ref, v_ref, values, slopes):
    ctrl = values.shape[1]
    vecs = u_ref.shape[-1]
    pair = 2 * ROWS
    area = ROWS * ROWS
    for lane in range(0, vecs, LANES):
        cols = slice(lane, lane + LANES)
        for j in range(0, ROWS, 2):
            tiles = {}

            def column(i, j):
                if (i, j) not in tiles:
                    tiles[i, j] = u_ref[i, j, :, cols]
                return tiles[i, j]

            for n, table in enumerate((slopes, values)):
                rows = []
                for k in range(j, min(j + 2, ctrl)):
                    rows += [terms(table, a, lambda i: column(i, k)), jnp.zeros((ROWS - ctrl, LANES), F32)]
                if j + 2 > ctrl:
                    rows.append(jnp.zeros(((j + 2 - ctrl) * ROWS, LANES), F32))
                high, low = split(jnp.concatenate(rows, axis=0))
                for part, block in enumerate((high, high, low)):
                    v_ref[a, n, part * area + j * ROWS : part * area + j * ROWS + pair, cols] = block


def gradient_stage(a, v_ref, wf_ref, g_ref):
    area = wf_ref.shape[0] // 3
    g_ref[a, 0:area] = jnp.dot(wf_ref[0:area], v_ref[a, 0], preferred_element_type=F32)
    plane = jnp.dot(wf_ref[...], v_ref[a, 1], preferred_element_type=F32)
    g_ref[a, area : 3 * area] = plane[area:]
    g_ref[a, 3 * area :] = plane[0:area]


def metric_stage(diag_ref, off_ref, weight_ref, t_ref):
    quad = weight_ref.shape[0]
    for f in range(3):
        t_ref[f, :, 0:quad] = diag_ref[f].T
        t_ref[3 + f, :, 0:quad] = off_ref[f].T
    t_ref[6, :, 0:quad] = weight_ref[...].T


def flux_stage(a, g_ref, t_ref, f_ref):
    area, vecs = t_ref.shape[1], g_ref.shape[-1]
    pair = 2 * ROWS
    for start in range(0, area, pair):
        d0, d1, d2, o0, o1, o2, w = (
            jnp.broadcast_to(t_ref[f, start : start + pair, a : a + 1], (pair, LANES)) for f in range(7)
        )
        for lane in range(0, vecs, LANES):
            cols = slice(lane, lane + LANES)
            gx, gy, gz, gp = (g_ref[a, n * area + start : n * area + start + pair, cols] for n in range(4))
            fluxes = (
                d0 * gx + o0 * gy + o1 * gz,
                o0 * gx + d1 * gy + o2 * gz,
                o1 * gx + o2 * gy + d2 * gz,
                w * gp,
            )
            for n, flux in enumerate(fluxes):
                high, low = split(flux)
                f_ref[a, n * area + start : n * area + start + pair, cols] = high
                f_ref[a, (4 + n) * area + start : (4 + n) * area + start + pair, cols] = low


def back_stage(a, f_ref, wb_ref, x_ref):
    half = f_ref.shape[1] // 2
    high, low = f_ref[a, 0:half], f_ref[a, half:]
    x_ref[a] = jnp.dot(wb_ref[...], jnp.concatenate([high, high, low], axis=0), preferred_element_type=F32)


def last_stage(x_ref, bulk_ref, values, slopes):
    ctrl = values.shape[1]
    area = ctrl * ROWS
    for j, lane in np.ndindex(ctrl, bulk_ref.shape[2]):
        cols = slice(lane * LANES, (lane + 1) * LANES)

        def block(kind):
            loaded = {}

            def at_plane(a):
                if a not in loaded:
                    loaded[a] = x_ref[a, kind * area + j * ROWS : kind * area + (j + 1) * ROWS, cols]
                return loaded[a]

            return at_plane

        by_x, by_rest, mass = block(0), block(1), block(2)
        for i in range(ctrl):
            bulk_ref[0, i, lane, j * ROWS : (j + 1) * ROWS] = terms(slopes.T, i, by_x) + terms(values.T, i, by_rest)
            bulk_ref[1, i, lane, j * ROWS : (j + 1) * ROWS] = terms(values.T, i, mass)


def scalars(flags_ref):
    flags = flags_ref[...]
    return [flags[0, d] for d in range(flags.shape[1])]


def turned(x, flag, ctrl):
    rows = lax.broadcasted_iota(jnp.int32, x.shape, 0)
    back = jnp.where(rows < ctrl, ctrl - 1 - rows, rows)
    return jnp.take_along_axis(x, jnp.where(flag == 1, back, rows), axis=0, mode="promise_in_bounds")


def at(index, flag, ctrl):
    return jnp.where(flag == 1, ctrl - 1 - index, index)


def body_kernel(values, slopes, flags_in, u_in, diag_in, off_in, weight_in, wf_in, wb_in,
                bulk_ref, xlow_ref, xhigh_ref, dlow_ref, dhigh_ref,
                flags_ref, u_ref, diag_ref, off_ref, weight_ref, wf_ref, wb_ref, u_sems, sems, t_ref, v_ref, g_ref, f_ref, x_ref):
    quad, ctrl = values.shape
    last = ctrl - 1
    small = [
        pltpu.make_async_copy(src, dst, sems.at[n])
        for n, (src, dst) in enumerate(
            ((wf_in, wf_ref), (diag_in, diag_ref), (off_in, off_ref), (weight_in, weight_ref), (wb_in, wb_ref), (flags_in, flags_ref))
        )
    ]
    planes = [pltpu.make_async_copy(u_in.at[i], u_ref.at[i], u_sems.at[i]) for i in range(ctrl)]
    for copy in small[1:4] + planes + small[:1] + small[4:]:
        copy.start()
    for copy in small[1:4]:
        copy.wait()
    metric_stage(diag_ref, off_ref, weight_ref, t_ref)
    for copy in planes + small[:1] + small[4:]:
        copy.wait()
    for step in range(quad + 2):
        if step < quad:
            operand_stage(step, u_ref, v_ref, values, slopes)
            gradient_stage(step, v_ref, wf_ref, g_ref)
        if 0 <= step - 1 < quad:
            flux_stage(step - 1, g_ref, t_ref, f_ref)
        if 0 <= step - 2 < quad:
            back_stage(step - 2, f_ref, wb_ref, x_ref)
    last_stage(x_ref, bulk_ref, values, slopes)
    lanes = bulk_ref.shape[2]
    flags = scalars(flags_ref)
    fi, fj, fk = flags
    for field, lane in np.ndindex(2, lanes):
        cols = pl.ds(lane * LANES, LANES)
        for i, x_ref in ((0, xlow_ref), (last, xhigh_ref)):
            here = at(i, fi, ctrl)
            for line, j in ((0, 0), (1, last)):
                x_ref[pl.ds((line * 2 + field) * ctrl, ctrl), cols] = y_line(bulk_ref, field, here, lane, j, flags, ctrl)
            for line, k in ((2, 0), (3, last)):
                x_ref[pl.ds((line * 2 + field) * ctrl, ctrl), cols] = z_line(bulk_ref, field, here, lane, k, flags, ctrl)
        for i, (side, j), (k, d_ref) in itertools.product(range(ctrl), ((0, 0), (1, last)), ((0, dlow_ref), (last, dhigh_ref))):
            row = at(j, fj, ctrl) * ROWS + at(k, fk, ctrl)
            d_ref[pl.ds((side * 2 + field) * ctrl + i, 1), cols] = bulk_ref[field, at(i, fi, ctrl), lane, pl.ds(row, 1), :]


def y_line(bulk_ref, field, here, lane, j, flags, ctrl):
    start = pl.multiple_of(at(j, flags[1], ctrl) * ROWS, ROWS)
    return turned(bulk_ref[field, here, lane, pl.ds(start, ROWS), :], flags[2], ctrl)[0:ctrl]


def z_line(bulk_ref, field, here, lane, k, flags, ctrl):
    block = bulk_ref[field, here, lane, pl.ds(at(k, flags[2], ctrl), ctrl, stride=ROWS), :]
    pad = jnp.zeros((ROWS - ctrl, LANES), F32)
    return turned(jnp.concatenate([block, pad], axis=0), flags[1], ctrl)[0:ctrl]


def pack_kernel(ctrl, flags_ref, bulk_ref, xlow_ref, xhigh_ref, y_ref, zlow_ref, zhigh_ref):
    flags = scalars(flags_ref)
    last = ctrl - 1
    for field, i, lane in np.ndindex(2, ctrl, bulk_ref.shape[2]):
        here = at(i, flags[0], ctrl)
        cols = pl.ds(lane * LANES, LANES)
        x_ref = xlow_ref if i == 0 else xhigh_ref if i == last else None

        def summed(block, line):
            return block if x_ref is None else block + x_ref[pl.ds((line * 2 + field) * ctrl, ctrl), cols]

        for side, j in ((0, 0), (1, last)):
            block = y_line(bulk_ref, field, here, lane, j, flags, ctrl)
            y_ref[pl.ds(((side * 2 + field) * ctrl + i) * ctrl, ctrl), cols] = summed(block, side)
        for side, k, z_ref in ((0, 0, zlow_ref), (1, last, zhigh_ref)):
            block = z_line(bulk_ref, field, here, lane, k, flags, ctrl)
            z_ref[pl.ds((field * ctrl + i) * ctrl, ctrl), cols] = summed(block, 2 + side)


def late_kernel(ctrl, flags_ref, bulk_ref, dlow_ref, dhigh_ref, low_ref, high_ref):
    flags = scalars(flags_ref)
    last = ctrl - 1
    inner = ctrl - 2
    for i, out_ref in ((0, low_ref), (last, high_ref)):
        here = at(i, flags[0], ctrl)
        for field, lane in np.ndindex(2, bulk_ref.shape[2]):
            cols = pl.ds(lane * LANES, LANES)
            for j in range(1, last):
                block = y_line(bulk_ref, field, here, lane, j, flags, ctrl)
                out_ref[pl.ds((field * inner + j - 1) * ctrl, ctrl), cols] = block
        for end, d_ref in enumerate((dlow_ref, dhigh_ref)):
            for side, field in np.ndindex(2, 2):
                row = 2 * inner * ctrl + (end * 2 + side) * 2 + field
                out_ref[pl.ds(row, 1), :] = d_ref[pl.ds((side * 2 + field) * ctrl + i, 1), :]


def join_kernel(ctrl, flags_ref, bulk_ref, xlow_ref, xhigh_ref, llow_ref, lhigh_ref, y_ref, zlow_ref, zhigh_ref,
                dlow_ref, dhigh_ref, k_out, n_out, stage_ref, sems):
    fi, fj, fk = scalars(flags_ref)
    last = ctrl - 1
    inner = ctrl - 2
    rows = lax.broadcasted_iota(jnp.int32, (ROWS, LANES), 0)
    at_low, at_high = rows == at(0, fk, ctrl), rows == at(last, fk, ctrl)
    pad = jnp.zeros((ROWS - ctrl, LANES), F32)
    copies = []

    def spread(row):
        return jnp.broadcast_to(row, (ROWS, LANES))

    for i, field in np.ndindex(ctrl, 2):
        here = at(i, fi, ctrl)
        x_ref, l_ref = (xlow_ref, llow_ref) if i == 0 else (xhigh_ref, lhigh_ref) if i == last else (None, None)
        for j, lane in np.ndindex(ctrl, bulk_ref.shape[2]):
            cols = pl.ds(lane * LANES, LANES)
            there = at(j, fj, ctrl)
            rim = 1 if j == 0 else 0 if j == last else None
            block = bulk_ref[field, here, lane, pl.ds(pl.multiple_of(there * ROWS, ROWS), ROWS), :]
            extra = []
            if x_ref is not None:
                if rim is None:
                    extra.append(l_ref[pl.ds((field * inner + j - 1) * ctrl, ctrl), cols])
                else:
                    extra.append(x_ref[pl.ds(((1 - rim) * 2 + field) * ctrl, ctrl), cols])
            if rim is not None:
                extra.append(y_ref[pl.ds(((rim * 2 + field) * ctrl + i) * ctrl, ctrl), cols])
            if extra:
                block = block + turned(jnp.concatenate([sum(extra[1:], extra[0]), pad], axis=0), fk, ctrl)
            ends = []
            for end, (z_ref, d_ref) in enumerate(((zlow_ref, dlow_ref), (zhigh_ref, dhigh_ref))):
                row = z_ref[pl.ds((field * ctrl + i) * ctrl + j, 1), cols]
                if rim is not None:
                    row = row + d_ref[pl.ds((rim * 2 + field) * ctrl + i, 1), cols]
                    if l_ref is not None:
                        row = row + l_ref[pl.ds(2 * inner * ctrl + (end * 2 + rim) * 2 + field, 1), cols]
                ends.append(spread(row))
            block = block + jnp.where(at_low, ends[0], jnp.where(at_high, ends[1], 0.0))
            stage_ref[field, i, there, :, cols] = block[0:ctrl]
        copy = pltpu.make_async_copy(stage_ref.at[field, i], (k_out, n_out)[field].at[here], sems.at[field, i])
        copy.start()
        copies.append(copy)
    for copy in copies:
        copy.wait()


def shifted(x, axes, sizes, steps):
    pairs = []
    for index in np.ndindex(*sizes):
        to = [(p + s) % n for p, s, n in zip(index, steps, sizes)]
        pairs.append((int(np.ravel_multi_index(index, sizes)), int(np.ravel_multi_index(to, sizes))))
    return lax.ppermute(x, axes, pairs)


def per_device(sizes, control_values, metric_diag, metric_off, mass_weight, orient):
    quad = mass_weight.shape[0]
    ctrl, vecs = control_values.shape[0], control_values.shape[-1]
    values, slopes = spline_tables(quad // 2)
    wf_np, wb_np = plane_tables(values, slopes)
    wf, wb = jnp.asarray(wf_np), jnp.asarray(wb_np)
    flags = orient.reshape(1, 3)
    hbm = pl.BlockSpec(memory_space=pltpu.HBM)
    vmem = pl.BlockSpec(memory_space=pltpu.VMEM)
    area = quad * quad
    nx, ny, nz = sizes
    face = 2 * ctrl * ctrl

    def sd(*shape):
        return jax.ShapeDtypeStruct(shape, F32)

    def call(kernel, mib, flops, **kwargs):
        def run(*args):
            return pl.pallas_call(
                kernel,
                compiler_params=pltpu.CompilerParams(vmem_limit_bytes=mib * 2**20),
                cost_estimate=pl.CostEstimate(flops=flops, bytes_accessed=10**6, transcendentals=0),
                **kwargs,
            )(*args)

        return run

    def crossed(pair, axes, counts, *steps):
        if ny == 2:
            return shifted(pair, axes, counts, (1, *steps))
        half = pair.shape[0] // 2
        return jnp.concatenate(
            [shifted(pair[:half], axes, counts, (-1, *steps)), shifted(pair[half:], axes, counts, (1, *steps))]
        )

    yz, yzn = ("py", "pz"), (ny, nz)
    inputs = (flags, control_values, metric_diag, metric_off, mass_weight, wf, wb)
    bulk, xlow, xhigh, dlow, dhigh = call(
        functools.partial(body_kernel, values, slopes),
        24,
        10**9,
        out_shape=[sd(2, ctrl, vecs // LANES, ctrl * ROWS, LANES)] + [sd(8 * ctrl, vecs)] * 2 + [sd(4 * ctrl, vecs)] * 2,
        in_specs=[hbm] * 7,
        out_specs=[vmem] * 5,
        scratch_shapes=[
            pltpu.VMEM((1, 3), jnp.int32),
            pltpu.VMEM(control_values.shape, F32),
            pltpu.VMEM(metric_diag.shape, F32),
            pltpu.VMEM(metric_off.shape, F32),
            pltpu.VMEM(mass_weight.shape, F32),
            pltpu.VMEM(wf.shape, BF16),
            pltpu.VMEM(wb.shape, BF16),
            pltpu.SemaphoreType.DMA((ctrl,)),
            pltpu.SemaphoreType.DMA((6,)),
            pltpu.VMEM((7, area, LANES), F32),
            pltpu.VMEM((quad, 2, 3 * ROWS * ROWS, vecs), BF16),
            pltpu.VMEM((quad, 4 * area, vecs), F32),
            pltpu.VMEM((quad, 8 * area, vecs), BF16),
            pltpu.VMEM((quad, 3 * ctrl * ROWS, vecs), F32),
        ],
    )(*(pltpu.with_memory_space_constraint(x, pltpu.HBM) for x in inputs))
    xlow_in = shifted(xhigh, ("px",), (nx,), (1,))
    xhigh_in = shifted(xlow, ("px",), (nx,), (-1,))
    dlow_in = crossed(dhigh, yz, yzn, 1)
    dhigh_in = crossed(dlow, yz, yzn, -1)
    ysend, zlow, zhigh = call(
        functools.partial(pack_kernel, ctrl),
        8,
        10**8,
        out_shape=[sd(2 * face, vecs)] + [sd(face, vecs)] * 2,
        in_specs=[vmem] + [vmem] * 3,
        out_specs=[vmem] * 3,
    )(flags, bulk, xlow_in, xhigh_in)
    zlow_in = shifted(zhigh, ("pz",), (nz,), (1,))
    y_in = crossed(ysend, ("py",), (ny,))
    zhigh_in = shifted(zlow, ("pz",), (nz,), (-1,))
    late = 2 * (ctrl - 2) * ctrl + 8
    llow, lhigh = call(
        functools.partial(late_kernel, ctrl),
        8,
        10**7,
        out_shape=[sd(late, vecs)] * 2,
        in_specs=[vmem] + [vmem] * 3,
        out_specs=[vmem] * 2,
    )(flags, bulk, dlow_in, dhigh_in)
    llow_in = shifted(lhigh, ("px",), (nx,), (1,))
    lhigh_in = shifted(llow, ("px",), (nx,), (-1,))
    return tuple(
        call(
            functools.partial(join_kernel, ctrl),
            10,
            10**8,
            out_shape=[sd(*control_values.shape)] * 2,
            in_specs=[vmem] + [vmem] * 10,
            out_specs=[hbm] * 2,
            scratch_shapes=[pltpu.VMEM((2, *control_values.shape), F32), pltpu.SemaphoreType.DMA((2, ctrl))],
        )(flags, bulk, xlow_in, xhigh_in, llow_in, lhigh_in, y_in, zlow_in, zhigh_in, dlow_in, dhigh_in)
    )


def solution(mesh):
    in_specs = (
        P("px", "py", "pz", None),
        P(None, "px", ("py", "pz")),
        P(None, "px", ("py", "pz")),
        P("px", ("py", "pz")),
        P("px", "py", "pz", None),
    )
    out_specs = (P("px", "py", "pz", None), P("px", "py", "pz", None))
    sizes = (mesh.shape["px"], mesh.shape["py"], mesh.shape["pz"])

    def body(*args):
        return per_device(sizes, *args)

    return jax.shard_map(body, mesh=mesh, in_specs=in_specs, out_specs=out_specs, check_vma=False)
```

```python
import functools
import itertools
import math

import jax
import jax.numpy as jnp
import numpy as np
from jax import lax
from jax.experimental import pallas as pl
from jax.experimental.pallas import tpu as pltpu
from jax.sharding import PartitionSpec as P


LANES = 128
ROWS = 8
F32 = jnp.float32
BF16 = jnp.bfloat16


def spline_tables(elements):
    knot_row = np.concatenate(
        [np.zeros(3), np.arange(elements + 1) * 1.0, np.full(3, float(elements))]
    )
    offsets = np.array([0.5 - 0.5 / math.sqrt(3.0), 0.5 + 0.5 / math.sqrt(3.0)])
    points = (np.arange(elements)[:, None] + offsets[None, :]).reshape(-1)
    intervals = np.repeat(np.arange(elements), 2) + 3
    current = np.zeros((points.size, knot_row.size - 1))
    current[np.arange(points.size), intervals] = 1.0
    previous = current
    for degree in range(1, 4):
        columns = knot_row.size - 1 - degree
        updated = np.zeros((points.size, columns))
        for i in range(columns):
            lower_gap = knot_row[i + degree] - knot_row[i]
            upper_gap = knot_row[i + degree + 1] - knot_row[i + 1]
            if lower_gap > 0:
                updated[:, i] += (points - knot_row[i]) / lower_gap * current[:, i]
            if upper_gap > 0:
                updated[:, i] += (knot_row[i + degree + 1] - points) / upper_gap * current[:, i + 1]
        previous = current
        current = updated
    slopes = np.zeros(current.shape)
    for i in range(current.shape[1]):
        lower_gap = knot_row[i + 3] - knot_row[i]
        upper_gap = knot_row[i + 4] - knot_row[i + 1]
        if lower_gap > 0:
            slopes[:, i] += 3.0 / lower_gap * previous[:, i]
        if upper_gap > 0:
            slopes[:, i] -= 3.0 / upper_gap * previous[:, i + 1]
    return (current.astype(np.float32), slopes.astype(np.float32))


def split(x):
    high = x.astype(BF16)
    return high, (x - high.astype(F32)).astype(BF16)


def split_np(x):
    high = x.astype(BF16)
    return high, (x - high.astype(np.float32)).astype(BF16)


def plane_tables(values, slopes):
    quad, ctrl = values.shape

    def pair(left, right):
        table = np.zeros((quad, quad, ROWS, ROWS), np.float32)
        table[:, :, :ctrl, :ctrl] = np.einsum("bj,ck->bcjk", left, right)
        return table.reshape(quad * quad, ROWS * ROWS)

    plain, by_y, by_z = pair(values, values), pair(slopes, values), pair(values, slopes)
    high, low = split_np(np.concatenate([plain, by_y, by_z]))
    forward = np.concatenate([high, low, high], axis=1)
    zero = np.zeros_like(plain.T)
    used = ctrl * ROWS
    back = np.concatenate(
        [
            np.concatenate([plain.T, zero, zero, zero], axis=1)[:used],
            np.concatenate([zero, by_y.T, by_z.T, zero], axis=1)[:used],
            np.concatenate([zero, zero, zero, plain.T], axis=1)[:used],
        ]
    )
    high, low = split_np(back)
    return forward, np.concatenate([high, low, high], axis=1)


def terms(table, index, column):
    total = None
    for n in range(table.shape[1]):
        if table[index, n] != 0.0:
            term = float(table[index, n]) * column(n)
            total = term if total is None else total + term
    return total


def operand_stage(a, u_ref, v_ref, values, slopes):
    ctrl = values.shape[1]
    vecs = u_ref.shape[-1]
    pair = 2 * ROWS
    area = ROWS * ROWS
    for lane in range(0, vecs, LANES):
        cols = slice(lane, lane + LANES)
        for j in range(0, ROWS, 2):
            tiles = {}

            def column(i, j):
                if (i, j) not in tiles:
                    tiles[i, j] = u_ref[i, j, :, cols]
                return tiles[i, j]

            for n, table in enumerate((slopes, values)):
                rows = []
                for k in range(j, min(j + 2, ctrl)):
                    rows += [terms(table, a, lambda i: column(i, k)), jnp.zeros((ROWS - ctrl, LANES), F32)]
                if j + 2 > ctrl:
                    rows.append(jnp.zeros(((j + 2 - ctrl) * ROWS, LANES), F32))
                high, low = split(jnp.concatenate(rows, axis=0))
                for part, block in enumerate((high, high, low)):
                    v_ref[a, n, part * area + j * ROWS : part * area + j * ROWS + pair, cols] = block


def gradient_stage(a, v_ref, wf_ref, g_ref):
    area = wf_ref.shape[0] // 3
    g_ref[a, 0:area] = jnp.dot(wf_ref[0:area], v_ref[a, 0], preferred_element_type=F32)
    plane = jnp.dot(wf_ref[...], v_ref[a, 1], preferred_element_type=F32)
    g_ref[a, area : 3 * area] = plane[area:]
    g_ref[a, 3 * area :] = plane[0:area]


def metric_stage(diag_ref, off_ref, weight_ref, t_ref):
    quad = weight_ref.shape[0]
    for f in range(3):
        t_ref[f, :, 0:quad] = diag_ref[f].T
        t_ref[3 + f, :, 0:quad] = off_ref[f].T
    t_ref[6, :, 0:quad] = weight_ref[...].T


def flux_stage(a, g_ref, t_ref, f_ref):
    area, vecs = t_ref.shape[1], g_ref.shape[-1]
    pair = 2 * ROWS
    for start in range(0, area, pair):
        d0, d1, d2, o0, o1, o2, w = (
            jnp.broadcast_to(t_ref[f, start : start + pair, a : a + 1], (pair, LANES)) for f in range(7)
        )
        for lane in range(0, vecs, LANES):
            cols = slice(lane, lane + LANES)
            gx, gy, gz, gp = (g_ref[a, n * area + start : n * area + start + pair, cols] for n in range(4))
            fluxes = (
                d0 * gx + o0 * gy + o1 * gz,
                o0 * gx + d1 * gy + o2 * gz,
                o1 * gx + o2 * gy + d2 * gz,
                w * gp,
            )
            for n, flux in enumerate(fluxes):
                high, low = split(flux)
                f_ref[a, n * area + start : n * area + start + pair, cols] = high
                f_ref[a, (4 + n) * area + start : (4 + n) * area + start + pair, cols] = low


def back_stage(a, f_ref, wb_ref, x_ref):
    half = f_ref.shape[1] // 2
    high, low = f_ref[a, 0:half], f_ref[a, half:]
    x_ref[a] = jnp.dot(wb_ref[...], jnp.concatenate([high, high, low], axis=0), preferred_element_type=F32)


def last_stage(x_ref, bulk_ref, values, slopes):
    ctrl = values.shape[1]
    area = ctrl * ROWS
    for j, lane in np.ndindex(ctrl, bulk_ref.shape[2]):
        cols = slice(lane * LANES, (lane + 1) * LANES)

        def block(kind):
            loaded = {}

            def at_plane(a):
                if a not in loaded:
                    loaded[a] = x_ref[a, kind * area + j * ROWS : kind * area + (j + 1) * ROWS, cols]
                return loaded[a]

            return at_plane

        by_x, by_rest, mass = block(0), block(1), block(2)
        for i in range(ctrl):
            bulk_ref[0, i, lane, j * ROWS : (j + 1) * ROWS] = terms(slopes.T, i, by_x) + terms(values.T, i, by_rest)
            bulk_ref[1, i, lane, j * ROWS : (j + 1) * ROWS] = terms(values.T, i, mass)


def scalars(flags_ref):
    flags = flags_ref[...]
    return [flags[0, d] for d in range(flags.shape[1])]


def turned(x, flag, ctrl):
    rows = lax.broadcasted_iota(jnp.int32, x.shape, 0)
    back = jnp.where(rows < ctrl, ctrl - 1 - rows, rows)
    return jnp.take_along_axis(x, jnp.where(flag == 1, back, rows), axis=0, mode="promise_in_bounds")


def at(index, flag, ctrl):
    return jnp.where(flag == 1, ctrl - 1 - index, index)


def body_kernel(values, slopes, flags_in, u_in, diag_in, off_in, weight_in, wf_in, wb_in,
                bulk_ref, xlow_ref, xhigh_ref, dlow_ref, dhigh_ref,
                flags_ref, u_ref, diag_ref, off_ref, weight_ref, wf_ref, wb_ref, u_sems, sems, t_ref, v_ref, g_ref, f_ref, x_ref):
    quad, ctrl = values.shape
    last = ctrl - 1
    small = [
        pltpu.make_async_copy(src, dst, sems.at[n])
        for n, (src, dst) in enumerate(
            ((wf_in, wf_ref), (diag_in, diag_ref), (off_in, off_ref), (weight_in, weight_ref), (wb_in, wb_ref), (flags_in, flags_ref))
        )
    ]
    planes = [pltpu.make_async_copy(u_in.at[i], u_ref.at[i], u_sems.at[i]) for i in range(ctrl)]
    for copy in small[1:4] + planes + small[:1] + small[4:]:
        copy.start()
    for copy in small[1:4]:
        copy.wait()
    metric_stage(diag_ref, off_ref, weight_ref, t_ref)
    for copy in planes + small[:1] + small[4:]:
        copy.wait()
    for step in range(quad + 2):
        if step < quad:
            operand_stage(step, u_ref, v_ref, values, slopes)
            gradient_stage(step, v_ref, wf_ref, g_ref)
        if 0 <= step - 1 < quad:
            flux_stage(step - 1, g_ref, t_ref, f_ref)
        if 0 <= step - 2 < quad:
            back_stage(step - 2, f_ref, wb_ref, x_ref)
    last_stage(x_ref, bulk_ref, values, slopes)
    lanes = bulk_ref.shape[2]
    flags = scalars(flags_ref)
    fi, fj, fk = flags
    for field, lane in np.ndindex(2, lanes):
        cols = pl.ds(lane * LANES, LANES)
        for i, x_ref in ((0, xlow_ref), (last, xhigh_ref)):
            here = at(i, fi, ctrl)
            for line, j in ((0, 0), (1, last)):
                x_ref[pl.ds((line * 2 + field) * ctrl, ctrl), cols] = y_line(bulk_ref, field, here, lane, j, flags, ctrl)
            for line, k in ((2, 0), (3, last)):
                x_ref[pl.ds((line * 2 + field) * ctrl, ctrl), cols] = z_line(bulk_ref, field, here, lane, k, flags, ctrl)
        for i, (side, j), (k, d_ref) in itertools.product(range(ctrl), ((0, 0), (1, last)), ((0, dlow_ref), (last, dhigh_ref))):
            row = at(j, fj, ctrl) * ROWS + at(k, fk, ctrl)
            d_ref[pl.ds(((side * lanes + lane) * 2 + field) * ctrl + i, 1), :] = bulk_ref[field, at(i, fi, ctrl), lane, pl.ds(row, 1), :]


def y_line(bulk_ref, field, here, lane, j, flags, ctrl):
    start = pl.multiple_of(at(j, flags[1], ctrl) * ROWS, ROWS)
    return turned(bulk_ref[field, here, lane, pl.ds(start, ROWS), :], flags[2], ctrl)[0:ctrl]


def z_line(bulk_ref, field, here, lane, k, flags, ctrl):
    block = bulk_ref[field, here, lane, pl.ds(at(k, flags[2], ctrl), ctrl, stride=ROWS), :]
    pad = jnp.zeros((ROWS - ctrl, LANES), F32)
    return turned(jnp.concatenate([block, pad], axis=0), flags[1], ctrl)[0:ctrl]


def pack_kernel(ctrl, flags_ref, bulk_ref, xlow_ref, xhigh_ref, y_ref, zlow_ref, zhigh_ref):
    flags = scalars(flags_ref)
    last = ctrl - 1
    lanes = bulk_ref.shape[2]
    for field, i, lane in np.ndindex(2, ctrl, lanes):
        here = at(i, flags[0], ctrl)
        cols = pl.ds(lane * LANES, LANES)
        x_ref = xlow_ref if i == 0 else xhigh_ref if i == last else None

        def summed(block, line):
            return block if x_ref is None else block + x_ref[pl.ds((line * 2 + field) * ctrl, ctrl), cols]

        for side, j in ((0, 0), (1, last)):
            block = y_line(bulk_ref, field, here, lane, j, flags, ctrl)
            y_ref[pl.ds((((side * lanes + lane) * 2 + field) * ctrl + i) * ctrl, ctrl), :] = summed(block, side)
        for side, k, z_ref in ((0, 0, zlow_ref), (1, last, zhigh_ref)):
            block = z_line(bulk_ref, field, here, lane, k, flags, ctrl)
            z_ref[pl.ds(((lane * 2 + field) * ctrl + i) * ctrl, ctrl), :] = summed(block, 2 + side)


def late_kernel(ctrl, flags_ref, bulk_ref, dlow_ref, dhigh_ref, low_ref, high_ref):
    flags = scalars(flags_ref)
    last = ctrl - 1
    inner = ctrl - 2
    lanes = bulk_ref.shape[2]
    count = 2 * inner * ctrl + 8
    for i, out_ref in ((0, low_ref), (last, high_ref)):
        here = at(i, flags[0], ctrl)
        for lane, field in np.ndindex(lanes, 2):
            for j in range(1, last):
                block = y_line(bulk_ref, field, here, lane, j, flags, ctrl)
                out_ref[pl.ds(lane * count + (field * inner + j - 1) * ctrl, ctrl), :] = block
            for end, d_ref in enumerate((dlow_ref, dhigh_ref)):
                for side in range(2):
                    row = lane * count + 2 * inner * ctrl + (end * 2 + side) * 2 + field
                    out_ref[pl.ds(row, 1), :] = d_ref[pl.ds(((side * lanes + lane) * 2 + field) * ctrl + i, 1), :]


def join_kernel(ctrl, flags_ref, bulk_ref, xlow_ref, xhigh_ref, llow_ref, lhigh_ref, y_ref, zlow_ref, zhigh_ref,
                dlow_ref, dhigh_ref, k_out, n_out, stage_ref, sems):
    fi, fj, fk = scalars(flags_ref)
    last = ctrl - 1
    inner = ctrl - 2
    rows = lax.broadcasted_iota(jnp.int32, (ROWS, LANES), 0)
    at_low, at_high = rows == at(0, fk, ctrl), rows == at(last, fk, ctrl)
    pad = jnp.zeros((ROWS - ctrl, LANES), F32)
    lanes = bulk_ref.shape[2]
    count = 2 * inner * ctrl + 8
    copies = []

    def spread(row):
        return jnp.broadcast_to(row, (ROWS, LANES))

    for i, field in np.ndindex(ctrl, 2):
        here = at(i, fi, ctrl)
        x_ref, l_ref = (xlow_ref, llow_ref) if i == 0 else (xhigh_ref, lhigh_ref) if i == last else (None, None)
        for j, lane in np.ndindex(ctrl, bulk_ref.shape[2]):
            cols = pl.ds(lane * LANES, LANES)
            there = at(j, fj, ctrl)
            rim = 1 if j == 0 else 0 if j == last else None
            block = bulk_ref[field, here, lane, pl.ds(pl.multiple_of(there * ROWS, ROWS), ROWS), :]
            extra = []
            if x_ref is not None:
                if rim is None:
                    extra.append(l_ref[pl.ds(lane * count + (field * inner + j - 1) * ctrl, ctrl), :])
                else:
                    extra.append(x_ref[pl.ds(((1 - rim) * 2 + field) * ctrl, ctrl), cols])
            if rim is not None:
                extra.append(y_ref[pl.ds((((rim * lanes + lane) * 2 + field) * ctrl + i) * ctrl, ctrl), :])
            if extra:
                block = block + turned(jnp.concatenate([sum(extra[1:], extra[0]), pad], axis=0), fk, ctrl)
            ends = []
            for end, (z_ref, d_ref) in enumerate(((zlow_ref, dlow_ref), (zhigh_ref, dhigh_ref))):
                row = z_ref[pl.ds(((lane * 2 + field) * ctrl + i) * ctrl + j, 1), :]
                if rim is not None:
                    row = row + d_ref[pl.ds(((rim * lanes + lane) * 2 + field) * ctrl + i, 1), :]
                    if l_ref is not None:
                        row = row + l_ref[pl.ds(lane * count + 2 * inner * ctrl + (end * 2 + rim) * 2 + field, 1), :]
                ends.append(spread(row))
            block = block + jnp.where(at_low, ends[0], jnp.where(at_high, ends[1], 0.0))
            stage_ref[field, i, there, :, cols] = block[0:ctrl]
        copy = pltpu.make_async_copy(stage_ref.at[field, i], (k_out, n_out)[field].at[here], sems.at[field, i])
        copy.start()
        copies.append(copy)
    for copy in copies:
        copy.wait()


def shifted(x, axes, sizes, steps):
    pairs = []
    for index in np.ndindex(*sizes):
        to = [(p + s) % n for p, s, n in zip(index, steps, sizes)]
        pairs.append((int(np.ravel_multi_index(index, sizes)), int(np.ravel_multi_index(to, sizes))))
    return lax.ppermute(x, axes, pairs)


def per_device(sizes, control_values, metric_diag, metric_off, mass_weight, orient):
    quad = mass_weight.shape[0]
    ctrl, vecs = control_values.shape[0], control_values.shape[-1]
    values, slopes = spline_tables(quad // 2)
    wf_np, wb_np = plane_tables(values, slopes)
    wf, wb = jnp.asarray(wf_np), jnp.asarray(wb_np)
    flags = orient.reshape(1, 3)
    hbm = pl.BlockSpec(memory_space=pltpu.HBM)
    vmem = pl.BlockSpec(memory_space=pltpu.VMEM)
    area = quad * quad
    nx, ny, nz = sizes
    face = 2 * ctrl * ctrl
    lanes = vecs // LANES

    def sd(*shape):
        return jax.ShapeDtypeStruct(shape, F32)

    def call(kernel, mib, flops, **kwargs):
        def run(*args):
            return pl.pallas_call(
                kernel,
                compiler_params=pltpu.CompilerParams(vmem_limit_bytes=mib * 2**20),
                cost_estimate=pl.CostEstimate(flops=flops, bytes_accessed=10**6, transcendentals=0),
                **kwargs,
            )(*args)

        return run

    def crossed(pair, axes, counts, *steps):
        if ny == 2:
            return shifted(pair, axes, counts, (1, *steps))
        half = pair.shape[0] // 2
        return jnp.concatenate(
            [shifted(pair[:half], axes, counts, (-1, *steps)), shifted(pair[half:], axes, counts, (1, *steps))]
        )

    yz, yzn = ("py", "pz"), (ny, nz)
    inputs = (flags, control_values, metric_diag, metric_off, mass_weight, wf, wb)
    bulk, xlow, xhigh, dlow, dhigh = call(
        functools.partial(body_kernel, values, slopes),
        24,
        10**9,
        out_shape=[sd(2, ctrl, vecs // LANES, ctrl * ROWS, LANES)] + [sd(8 * ctrl, vecs)] * 2 + [sd(4 * ctrl * lanes, LANES)] * 2,
        in_specs=[hbm] * 7,
        out_specs=[vmem] * 5,
        scratch_shapes=[
            pltpu.VMEM((1, 3), jnp.int32),
            pltpu.VMEM(control_values.shape, F32),
            pltpu.VMEM(metric_diag.shape, F32),
            pltpu.VMEM(metric_off.shape, F32),
            pltpu.VMEM(mass_weight.shape, F32),
            pltpu.VMEM(wf.shape, BF16),
            pltpu.VMEM(wb.shape, BF16),
            pltpu.SemaphoreType.DMA((ctrl,)),
            pltpu.SemaphoreType.DMA((6,)),
            pltpu.VMEM((7, area, LANES), F32),
            pltpu.VMEM((quad, 2, 3 * ROWS * ROWS, vecs), BF16),
            pltpu.VMEM((quad, 4 * area, vecs), F32),
            pltpu.VMEM((quad, 8 * area, vecs), BF16),
            pltpu.VMEM((quad, 3 * ctrl * ROWS, vecs), F32),
        ],
    )(*(pltpu.with_memory_space_constraint(x, pltpu.HBM) for x in inputs))
    xlow_in = shifted(xhigh, ("px",), (nx,), (1,))
    xhigh_in = shifted(xlow, ("px",), (nx,), (-1,))
    dlow_in = crossed(dhigh, yz, yzn, 1)
    dhigh_in = crossed(dlow, yz, yzn, -1)
    ysend, zlow, zhigh = call(
        functools.partial(pack_kernel, ctrl),
        8,
        10**8,
        out_shape=[sd(2 * face * lanes, LANES)] + [sd(face * lanes, LANES)] * 2,
        in_specs=[vmem] + [vmem] * 3,
        out_specs=[vmem] * 3,
    )(flags, bulk, xlow_in, xhigh_in)
    zlow_in = shifted(zhigh, ("pz",), (nz,), (1,))
    y_in = crossed(ysend, ("py",), (ny,))
    zhigh_in = shifted(zlow, ("pz",), (nz,), (-1,))
    late = 2 * (ctrl - 2) * ctrl + 8
    llow, lhigh = call(
        functools.partial(late_kernel, ctrl),
        8,
        10**7,
        out_shape=[sd(late * lanes, LANES)] * 2,
        in_specs=[vmem] + [vmem] * 3,
        out_specs=[vmem] * 2,
    )(flags, bulk, dlow_in, dhigh_in)
    llow_in = shifted(lhigh, ("px",), (nx,), (1,))
    lhigh_in = shifted(llow, ("px",), (nx,), (-1,))
    return tuple(
        call(
            functools.partial(join_kernel, ctrl),
            10,
            10**8,
            out_shape=[sd(*control_values.shape)] * 2,
            in_specs=[vmem] + [vmem] * 10,
            out_specs=[hbm] * 2,
            scratch_shapes=[pltpu.VMEM((2, *control_values.shape), F32), pltpu.SemaphoreType.DMA((2, ctrl))],
        )(flags, bulk, xlow_in, xhigh_in, llow_in, lhigh_in, y_in, zlow_in, zhigh_in, dlow_in, dhigh_in)
    )


def solution(mesh):
    in_specs = (
        P("px", "py", "pz", None),
        P(None, "px", ("py", "pz")),
        P(None, "px", ("py", "pz")),
        P("px", ("py", "pz")),
        P("px", "py", "pz", None),
    )
    out_specs = (P("px", "py", "pz", None), P("px", "py", "pz", None))
    sizes = (mesh.shape["px"], mesh.shape["py"], mesh.shape["pz"])

    def body(*args):
        return per_device(sizes, *args)

    return jax.shard_map(body, mesh=mesh, in_specs=in_specs, out_specs=out_specs, check_vma=False)
```

```python
import functools
import itertools
import math

import jax
import jax.numpy as jnp
import numpy as np
from jax import lax
from jax.experimental import pallas as pl
from jax.experimental.pallas import tpu as pltpu
from jax.sharding import PartitionSpec as P


LANES = 128
ROWS = 8
F32 = jnp.float32
BF16 = jnp.bfloat16


def spline_tables(elements):
    knot_row = np.concatenate(
        [np.zeros(3), np.arange(elements + 1) * 1.0, np.full(3, float(elements))]
    )
    offsets = np.array([0.5 - 0.5 / math.sqrt(3.0), 0.5 + 0.5 / math.sqrt(3.0)])
    points = (np.arange(elements)[:, None] + offsets[None, :]).reshape(-1)
    intervals = np.repeat(np.arange(elements), 2) + 3
    current = np.zeros((points.size, knot_row.size - 1))
    current[np.arange(points.size), intervals] = 1.0
    previous = current
    for degree in range(1, 4):
        columns = knot_row.size - 1 - degree
        updated = np.zeros((points.size, columns))
        for i in range(columns):
            lower_gap = knot_row[i + degree] - knot_row[i]
            upper_gap = knot_row[i + degree + 1] - knot_row[i + 1]
            if lower_gap > 0:
                updated[:, i] += (points - knot_row[i]) / lower_gap * current[:, i]
            if upper_gap > 0:
                updated[:, i] += (knot_row[i + degree + 1] - points) / upper_gap * current[:, i + 1]
        previous = current
        current = updated
    slopes = np.zeros(current.shape)
    for i in range(current.shape[1]):
        lower_gap = knot_row[i + 3] - knot_row[i]
        upper_gap = knot_row[i + 4] - knot_row[i + 1]
        if lower_gap > 0:
            slopes[:, i] += 3.0 / lower_gap * previous[:, i]
        if upper_gap > 0:
            slopes[:, i] -= 3.0 / upper_gap * previous[:, i + 1]
    return (current.astype(np.float32), slopes.astype(np.float32))


def split(x):
    high = x.astype(BF16)
    return high, (x - high.astype(F32)).astype(BF16)


def split_np(x):
    high = x.astype(BF16)
    return high, (x - high.astype(np.float32)).astype(BF16)


def plane_tables(values, slopes):
    quad, ctrl = values.shape

    def pair(left, right):
        table = np.zeros((quad, quad, ROWS, ROWS), np.float32)
        table[:, :, :ctrl, :ctrl] = np.einsum("bj,ck->bcjk", left, right)
        return table.reshape(quad * quad, ROWS * ROWS)

    plain, by_y, by_z = pair(values, values), pair(slopes, values), pair(values, slopes)
    high, low = split_np(np.concatenate([plain, by_y, by_z]))
    forward = np.concatenate([high, low, high], axis=1)
    zero = np.zeros_like(plain.T)
    used = ctrl * ROWS
    back = np.concatenate(
        [
            np.concatenate([plain.T, zero, zero, zero], axis=1)[:used],
            np.concatenate([zero, by_y.T, by_z.T, zero], axis=1)[:used],
            np.concatenate([zero, zero, zero, plain.T], axis=1)[:used],
        ]
    )
    high, low = split_np(back)
    return forward, np.concatenate([high, low, high], axis=1)


def terms(table, index, column):
    total = None
    for n in range(table.shape[1]):
        if table[index, n] != 0.0:
            term = float(table[index, n]) * column(n)
            total = term if total is None else total + term
    return total


def operand_stage(a, u_ref, v_ref, values, slopes):
    ctrl = values.shape[1]
    vecs = u_ref.shape[-1]
    pair = 2 * ROWS
    area = ROWS * ROWS
    for lane in range(0, vecs, LANES):
        cols = slice(lane, lane + LANES)
        for j in range(0, ROWS, 2):
            tiles = {}

            def column(i, j):
                if (i, j) not in tiles:
                    tiles[i, j] = u_ref[i, j, :, cols]
                return tiles[i, j]

            for n, table in enumerate((slopes, values)):
                rows = []
                for k in range(j, min(j + 2, ctrl)):
                    rows += [terms(table, a, lambda i: column(i, k)), jnp.zeros((ROWS - ctrl, LANES), F32)]
                if j + 2 > ctrl:
                    rows.append(jnp.zeros(((j + 2 - ctrl) * ROWS, LANES), F32))
                high, low = split(jnp.concatenate(rows, axis=0))
                for part, block in enumerate((high, high, low)):
                    v_ref[a, n, part * area + j * ROWS : part * area + j * ROWS + pair, cols] = block


def gradient_stage(a, v_ref, wf_ref, g_ref):
    area = wf_ref.shape[0] // 3
    g_ref[a, 0:area] = jnp.dot(wf_ref[0:area], v_ref[a, 0], preferred_element_type=F32)
    plane = jnp.dot(wf_ref[...], v_ref[a, 1], preferred_element_type=F32)
    g_ref[a, area : 3 * area] = plane[area:]
    g_ref[a, 3 * area :] = plane[0:area]


def metric_stage(diag_ref, off_ref, weight_ref, t_ref):
    quad = weight_ref.shape[0]
    for f in range(3):
        t_ref[f, :, 0:quad] = diag_ref[f].T
        t_ref[3 + f, :, 0:quad] = off_ref[f].T
    t_ref[6, :, 0:quad] = weight_ref[...].T


def flux_stage(a, g_ref, t_ref, f_ref):
    area, vecs = t_ref.shape[1], g_ref.shape[-1]
    pair = 2 * ROWS
    for start in range(0, area, pair):
        d0, d1, d2, o0, o1, o2, w = (
            jnp.broadcast_to(t_ref[f, start : start + pair, a : a + 1], (pair, LANES)) for f in range(7)
        )
        for lane in range(0, vecs, LANES):
            cols = slice(lane, lane + LANES)
            gx, gy, gz, gp = (g_ref[a, n * area + start : n * area + start + pair, cols] for n in range(4))
            fluxes = (
                d0 * gx + o0 * gy + o1 * gz,
                o0 * gx + d1 * gy + o2 * gz,
                o1 * gx + o2 * gy + d2 * gz,
                w * gp,
            )
            for n, flux in enumerate(fluxes):
                high, low = split(flux)
                f_ref[a, n * area + start : n * area + start + pair, cols] = high
                f_ref[a, (4 + n) * area + start : (4 + n) * area + start + pair, cols] = low


def back_stage(a, f_ref, wb_ref, x_ref):
    half = f_ref.shape[1] // 2
    high, low = f_ref[a, 0:half], f_ref[a, half:]
    x_ref[a] = jnp.dot(wb_ref[...], jnp.concatenate([high, high, low], axis=0), preferred_element_type=F32)


def last_stage(x_ref, bulk_ref, values, slopes):
    ctrl = values.shape[1]
    area = ctrl * ROWS
    for j, lane in np.ndindex(ctrl, bulk_ref.shape[2]):
        cols = slice(lane * LANES, (lane + 1) * LANES)

        def block(kind):
            loaded = {}

            def at_plane(a):
                if a not in loaded:
                    loaded[a] = x_ref[a, kind * area + j * ROWS : kind * area + (j + 1) * ROWS, cols]
                return loaded[a]

            return at_plane

        by_x, by_rest, mass = block(0), block(1), block(2)
        for i in range(ctrl):
            bulk_ref[0, i, lane, j * ROWS : (j + 1) * ROWS] = terms(slopes.T, i, by_x) + terms(values.T, i, by_rest)
            bulk_ref[1, i, lane, j * ROWS : (j + 1) * ROWS] = terms(values.T, i, mass)


def scalars(flags_ref):
    flags = flags_ref[...]
    return [flags[0, d] for d in range(flags.shape[1])]


def turned(x, flag, ctrl):
    rows = lax.broadcasted_iota(jnp.int32, x.shape, 0)
    back = jnp.where(rows < ctrl, ctrl - 1 - rows, rows)
    return jnp.take_along_axis(x, jnp.where(flag == 1, back, rows), axis=0, mode="promise_in_bounds")


def at(index, flag, ctrl):
    return jnp.where(flag == 1, ctrl - 1 - index, index)


def body_kernel(values, slopes, flags_in, u_in, diag_in, off_in, weight_in, wf_in, wb_in,
                bulk_ref, xlow_ref, xhigh_ref, dlow_ref, dhigh_ref,
                flags_ref, u_ref, diag_ref, off_ref, weight_ref, wf_ref, wb_ref, u_sems, sems, t_ref, v_ref, g_ref, f_ref, x_ref):
    quad, ctrl = values.shape
    last = ctrl - 1
    small = [
        pltpu.make_async_copy(src, dst, sems.at[n])
        for n, (src, dst) in enumerate(
            ((wf_in, wf_ref), (diag_in, diag_ref), (off_in, off_ref), (weight_in, weight_ref), (wb_in, wb_ref), (flags_in, flags_ref))
        )
    ]
    planes = [pltpu.make_async_copy(u_in.at[i], u_ref.at[i], u_sems.at[i]) for i in range(ctrl)]
    for copy in small[:4] + planes + small[4:]:
        copy.start()
    for copy in small[1:4]:
        copy.wait()
    metric_stage(diag_ref, off_ref, weight_ref, t_ref)
    needed = max(i for i in range(ctrl) if values[:2, i].any() or slopes[:2, i].any()) + 1
    for copy in small[:1] + planes[:needed]:
        copy.wait()
    for step in range(quad + 2):
        if step == 2:
            for copy in planes[needed:] + small[4:]:
                copy.wait()
        if step < quad:
            operand_stage(step, u_ref, v_ref, values, slopes)
            gradient_stage(step, v_ref, wf_ref, g_ref)
        if 0 <= step - 1 < quad:
            flux_stage(step - 1, g_ref, t_ref, f_ref)
        if 0 <= step - 2 < quad:
            back_stage(step - 2, f_ref, wb_ref, x_ref)
    last_stage(x_ref, bulk_ref, values, slopes)
    lanes = bulk_ref.shape[2]
    flags = scalars(flags_ref)
    fi, fj, fk = flags
    for field, lane in np.ndindex(2, lanes):
        cols = pl.ds(lane * LANES, LANES)
        for i, x_ref in ((0, xlow_ref), (last, xhigh_ref)):
            here = at(i, fi, ctrl)
            for line, j in ((0, 0), (1, last)):
                x_ref[pl.ds((line * 2 + field) * ctrl, ctrl), cols] = y_line(bulk_ref, field, here, lane, j, flags, ctrl)
            for line, k in ((2, 0), (3, last)):
                x_ref[pl.ds((line * 2 + field) * ctrl, ctrl), cols] = z_line(bulk_ref, field, here, lane, k, flags, ctrl)
        for i, (side, j), (k, d_ref) in itertools.product(range(ctrl), ((0, 0), (1, last)), ((0, dlow_ref), (last, dhigh_ref))):
            row = at(j, fj, ctrl) * ROWS + at(k, fk, ctrl)
            d_ref[pl.ds(((side * lanes + lane) * 2 + field) * ctrl + i, 1), :] = bulk_ref[field, at(i, fi, ctrl), lane, pl.ds(row, 1), :]


def y_line(bulk_ref, field, here, lane, j, flags, ctrl):
    start = pl.multiple_of(at(j, flags[1], ctrl) * ROWS, ROWS)
    return turned(bulk_ref[field, here, lane, pl.ds(start, ROWS), :], flags[2], ctrl)[0:ctrl]


def z_line(bulk_ref, field, here, lane, k, flags, ctrl):
    block = bulk_ref[field, here, lane, pl.ds(at(k, flags[2], ctrl), ctrl, stride=ROWS), :]
    pad = jnp.zeros((ROWS - ctrl, LANES), F32)
    return turned(jnp.concatenate([block, pad], axis=0), flags[1], ctrl)[0:ctrl]


def pack_kernel(ctrl, flags_ref, bulk_ref, xlow_ref, xhigh_ref, y_ref, zlow_ref, zhigh_ref):
    flags = scalars(flags_ref)
    last = ctrl - 1
    lanes = bulk_ref.shape[2]
    for field, i, lane in np.ndindex(2, ctrl, lanes):
        here = at(i, flags[0], ctrl)
        cols = pl.ds(lane * LANES, LANES)
        x_ref = xlow_ref if i == 0 else xhigh_ref if i == last else None

        def summed(block, line):
            return block if x_ref is None else block + x_ref[pl.ds((line * 2 + field) * ctrl, ctrl), cols]

        for side, j in ((0, 0), (1, last)):
            block = y_line(bulk_ref, field, here, lane, j, flags, ctrl)
            y_ref[pl.ds((((side * lanes + lane) * 2 + field) * ctrl + i) * ctrl, ctrl), :] = summed(block, side)
        for side, k, z_ref in ((0, 0, zlow_ref), (1, last, zhigh_ref)):
            block = z_line(bulk_ref, field, here, lane, k, flags, ctrl)
            z_ref[pl.ds(((lane * 2 + field) * ctrl + i) * ctrl, ctrl), :] = summed(block, 2 + side)


def late_kernel(ctrl, flags_ref, bulk_ref, dlow_ref, dhigh_ref, low_ref, high_ref):
    flags = scalars(flags_ref)
    last = ctrl - 1
    inner = ctrl - 2
    lanes = bulk_ref.shape[2]
    count = 2 * inner * ctrl + 8
    for i, out_ref in ((0, low_ref), (last, high_ref)):
        here = at(i, flags[0], ctrl)
        for lane, field in np.ndindex(lanes, 2):
            for j in range(1, last):
                block = y_line(bulk_ref, field, here, lane, j, flags, ctrl)
                out_ref[pl.ds(lane * count + (field * inner + j - 1) * ctrl, ctrl), :] = block
            for end, d_ref in enumerate((dlow_ref, dhigh_ref)):
                for side in range(2):
                    row = lane * count + 2 * inner * ctrl + (end * 2 + side) * 2 + field
                    out_ref[pl.ds(row, 1), :] = d_ref[pl.ds(((side * lanes + lane) * 2 + field) * ctrl + i, 1), :]


def join_kernel(ctrl, flags_ref, bulk_ref, xlow_ref, xhigh_ref, llow_ref, lhigh_ref, y_ref, zlow_ref, zhigh_ref,
                dlow_ref, dhigh_ref, k_out, n_out, stage_ref, sems):
    fi, fj, fk = scalars(flags_ref)
    last = ctrl - 1
    inner = ctrl - 2
    rows = lax.broadcasted_iota(jnp.int32, (ROWS, LANES), 0)
    at_low, at_high = rows == at(0, fk, ctrl), rows == at(last, fk, ctrl)
    pad = jnp.zeros((ROWS - ctrl, LANES), F32)
    lanes = bulk_ref.shape[2]
    count = 2 * inner * ctrl + 8
    copies = []

    def spread(row):
        return jnp.broadcast_to(row, (ROWS, LANES))

    for i, field in np.ndindex(ctrl, 2):
        here = at(i, fi, ctrl)
        x_ref, l_ref = (xlow_ref, llow_ref) if i == 0 else (xhigh_ref, lhigh_ref) if i == last else (None, None)
        for j, lane in np.ndindex(ctrl, bulk_ref.shape[2]):
            cols = pl.ds(lane * LANES, LANES)
            there = at(j, fj, ctrl)
            rim = 1 if j == 0 else 0 if j == last else None
            block = bulk_ref[field, here, lane, pl.ds(pl.multiple_of(there * ROWS, ROWS), ROWS), :]
            extra = []
            if x_ref is not None:
                if rim is None:
                    extra.append(l_ref[pl.ds(lane * count + (field * inner + j - 1) * ctrl, ctrl), :])
                else:
                    extra.append(x_ref[pl.ds(((1 - rim) * 2 + field) * ctrl, ctrl), cols])
            if rim is not None:
                extra.append(y_ref[pl.ds((((rim * lanes + lane) * 2 + field) * ctrl + i) * ctrl, ctrl), :])
            if extra:
                block = block + turned(jnp.concatenate([sum(extra[1:], extra[0]), pad], axis=0), fk, ctrl)
            ends = []
            for end, (z_ref, d_ref) in enumerate(((zlow_ref, dlow_ref), (zhigh_ref, dhigh_ref))):
                row = z_ref[pl.ds(((lane * 2 + field) * ctrl + i) * ctrl + j, 1), :]
                if rim is not None:
                    row = row + d_ref[pl.ds(((rim * lanes + lane) * 2 + field) * ctrl + i, 1), :]
                    if l_ref is not None:
                        row = row + l_ref[pl.ds(lane * count + 2 * inner * ctrl + (end * 2 + rim) * 2 + field, 1), :]
                ends.append(spread(row))
            block = block + jnp.where(at_low, ends[0], jnp.where(at_high, ends[1], 0.0))
            stage_ref[field, i, there, :, cols] = block[0:ctrl]
        copy = pltpu.make_async_copy(stage_ref.at[field, i], (k_out, n_out)[field].at[here], sems.at[field, i])
        copy.start()
        copies.append(copy)
    for copy in copies:
        copy.wait()


def shifted(x, axes, sizes, steps):
    pairs = []
    for index in np.ndindex(*sizes):
        to = [(p + s) % n for p, s, n in zip(index, steps, sizes)]
        pairs.append((int(np.ravel_multi_index(index, sizes)), int(np.ravel_multi_index(to, sizes))))
    return lax.ppermute(x, axes, pairs)


def per_device(sizes, control_values, metric_diag, metric_off, mass_weight, orient):
    quad = mass_weight.shape[0]
    ctrl, vecs = control_values.shape[0], control_values.shape[-1]
    values, slopes = spline_tables(quad // 2)
    wf_np, wb_np = plane_tables(values, slopes)
    wf, wb = jnp.asarray(wf_np), jnp.asarray(wb_np)
    flags = orient.reshape(1, 3)
    hbm = pl.BlockSpec(memory_space=pltpu.HBM)
    vmem = pl.BlockSpec(memory_space=pltpu.VMEM)
    area = quad * quad
    nx, ny, nz = sizes
    face = 2 * ctrl * ctrl
    lanes = vecs // LANES

    def sd(*shape):
        return jax.ShapeDtypeStruct(shape, F32)

    def call(kernel, mib, flops, **kwargs):
        def run(*args):
            return pl.pallas_call(
                kernel,
                compiler_params=pltpu.CompilerParams(vmem_limit_bytes=mib * 2**20),
                cost_estimate=pl.CostEstimate(flops=flops, bytes_accessed=10**6, transcendentals=0),
                **kwargs,
            )(*args)

        return run

    def crossed(pair, axes, counts, *steps):
        if ny == 2:
            return shifted(pair, axes, counts, (1, *steps))
        half = pair.shape[0] // 2
        return jnp.concatenate(
            [shifted(pair[:half], axes, counts, (-1, *steps)), shifted(pair[half:], axes, counts, (1, *steps))]
        )

    yz, yzn = ("py", "pz"), (ny, nz)
    inputs = (flags, control_values, metric_diag, metric_off, mass_weight, wf, wb)
    bulk, xlow, xhigh, dlow, dhigh = call(
        functools.partial(body_kernel, values, slopes),
        24,
        10**9,
        out_shape=[sd(2, ctrl, vecs // LANES, ctrl * ROWS, LANES)] + [sd(8 * ctrl, vecs)] * 2 + [sd(4 * ctrl * lanes, LANES)] * 2,
        in_specs=[hbm] * 7,
        out_specs=[vmem] * 5,
        scratch_shapes=[
            pltpu.VMEM((1, 3), jnp.int32),
            pltpu.VMEM(control_values.shape, F32),
            pltpu.VMEM(metric_diag.shape, F32),
            pltpu.VMEM(metric_off.shape, F32),
            pltpu.VMEM(mass_weight.shape, F32),
            pltpu.VMEM(wf.shape, BF16),
            pltpu.VMEM(wb.shape, BF16),
            pltpu.SemaphoreType.DMA((ctrl,)),
            pltpu.SemaphoreType.DMA((6,)),
            pltpu.VMEM((7, area, LANES), F32),
            pltpu.VMEM((quad, 2, 3 * ROWS * ROWS, vecs), BF16),
            pltpu.VMEM((quad, 4 * area, vecs), F32),
            pltpu.VMEM((quad, 8 * area, vecs), BF16),
            pltpu.VMEM((quad, 3 * ctrl * ROWS, vecs), F32),
        ],
    )(*(pltpu.with_memory_space_constraint(x, pltpu.HBM) for x in inputs))
    xlow_in = shifted(xhigh, ("px",), (nx,), (1,))
    xhigh_in = shifted(xlow, ("px",), (nx,), (-1,))
    dlow_in = crossed(dhigh, yz, yzn, 1)
    dhigh_in = crossed(dlow, yz, yzn, -1)
    ysend, zlow, zhigh = call(
        functools.partial(pack_kernel, ctrl),
        8,
        10**8,
        out_shape=[sd(2 * face * lanes, LANES)] + [sd(face * lanes, LANES)] * 2,
        in_specs=[vmem] + [vmem] * 3,
        out_specs=[vmem] * 3,
    )(flags, bulk, xlow_in, xhigh_in)
    zlow_in = shifted(zhigh, ("pz",), (nz,), (1,))
    y_in = crossed(ysend, ("py",), (ny,))
    zhigh_in = shifted(zlow, ("pz",), (nz,), (-1,))
    late = 2 * (ctrl - 2) * ctrl + 8
    llow, lhigh = call(
        functools.partial(late_kernel, ctrl),
        8,
        10**7,
        out_shape=[sd(late * lanes, LANES)] * 2,
        in_specs=[vmem] + [vmem] * 3,
        out_specs=[vmem] * 2,
    )(flags, bulk, dlow_in, dhigh_in)
    llow_in = shifted(lhigh, ("px",), (nx,), (1,))
    lhigh_in = shifted(llow, ("px",), (nx,), (-1,))
    return tuple(
        call(
            functools.partial(join_kernel, ctrl),
            10,
            10**8,
            out_shape=[sd(*control_values.shape)] * 2,
            in_specs=[vmem] + [vmem] * 10,
            out_specs=[hbm] * 2,
            scratch_shapes=[pltpu.VMEM((2, *control_values.shape), F32), pltpu.SemaphoreType.DMA((2, ctrl))],
        )(flags, bulk, xlow_in, xhigh_in, llow_in, lhigh_in, y_in, zlow_in, zhigh_in, dlow_in, dhigh_in)
    )


def solution(mesh):
    in_specs = (
        P("px", "py", "pz", None),
        P(None, "px", ("py", "pz")),
        P(None, "px", ("py", "pz")),
        P("px", ("py", "pz")),
        P("px", "py", "pz", None),
    )
    out_specs = (P("px", "py", "pz", None), P("px", "py", "pz", None))
    sizes = (mesh.shape["px"], mesh.shape["py"], mesh.shape["pz"])

    def body(*args):
        return per_device(sizes, *args)

    return jax.shard_map(body, mesh=mesh, in_specs=in_specs, out_specs=out_specs, check_vma=False)
```
